256 devices in a mesh: vocab: 64 (over x, z, core), seq: 4 (over y).
Axes of the slice: x: 4, y: 4, z: 8, core: 2. Of those that a mesh axis runs over, the one named last changes fastest.
Arguments:
- hidden: bfloat16 [4096, 4096], P(('vocab', 'seq')), may hold values from -40 to 40
- embedding: bfloat16 [65536, 4096], P('vocab'), may hold values from -40 to 40
- logit_scale: float32 [65536], P('vocab'), may hold values from 100 to 600
- targets: int32 [4096], P(('vocab', 'seq')), may hold values from 0 to 65535
Outputs:
- token_loss: float32 [4096], P(('vocab', 'seq'))
- mean_loss: float32 [], replicated
The draws below stay inside these ranges and needn't reach their ends.
All inputs are finite; a program needn't handle non-finite values.
Results may differ from the reference program's by a relative error of at most 0.0012.
Values may be sent and summed in bfloat16 or wider, within the bound.
No kernel may reach another device: no remote copies, remote signals or barrier semaphores. Data moves between devices by JAX's collectives and lax.ppermute only.
A program may use at most 64 MiB of HBM per device.

```python
import math
import jax
import jax.numpy as jnp
from jax import lax

D = 4096
V_DEV = 1024
VOCAB = 65536
TOKENS = 4096


def draw_embedding(key, part):
    values = jnp.clip(jax.random.normal(jax.random.fold_in(key, 11), (VOCAB, D), jnp.float32), -4.0, 4.0)
    return values.astype(jnp.bfloat16)


def draw_hidden(key, part):
    values = jnp.clip(jax.random.normal(jax.random.fold_in(key, 21), (TOKENS, D), jnp.float32), -4.0, 4.0)
    return values.astype(jnp.bfloat16)


def draw_logit_scale(key, part):
    rising = 1.0 + 0.25 * jnp.arange(VOCAB, dtype=jnp.float32) / VOCAB
    values = jnp.exp(jax.random.uniform(jax.random.fold_in(key, 32), (VOCAB,), jnp.float32, math.log(150.0), math.log(250.0))) * rising
    return values.astype(jnp.float32)


def touch_ends(array, stream_key, smallest, top_value):
    longest = array.shape.index(max(array.shape))
    spots = []
    for shift in (0, 1):
        where = [jax.random.randint(jax.random.fold_in(stream_key, axis), (), 0, length) for axis, length in enumerate(array.shape)]
        where[longest] = (where[longest] + shift) % array.shape[longest]
        spots.append(tuple(where))
    return array.at[spots[0]].set(smallest).at[spots[1]].set(top_value)


def setup_inputs(seed: int = 0) -> dict:
    seeds = jax.random.split(jax.random.key(seed), 5)
    hidden = draw_hidden(jax.random.fold_in(seeds[4], 71), 0)
    embedding = draw_embedding(jax.random.fold_in(seeds[4], 71), 0)
    logit_scale = draw_logit_scale(jax.random.fold_in(seeds[4], 71), 0)
    targets = touch_ends(jax.random.randint(seeds[3], (TOKENS,), 0, VOCAB), jax.random.fold_in(seeds[3], 1), 0, VOCAB - 1).astype(jnp.int32)
    return {"hidden": hidden, "embedding": embedding, "logit_scale": logit_scale, "targets": targets}


epsilon = 1e-06

def reference(hidden, embedding, logit_scale, targets):
    hidden_wide = hidden.astype(jnp.float32)
    hidden_unit = (hidden_wide * lax.rsqrt(lax.optimization_barrier(jnp.sum(hidden_wide * hidden_wide, axis=1, keepdims=True)) + epsilon)).astype(jnp.bfloat16)
    block_count = VOCAB // V_DEV
    embed_blocks = embedding.reshape(block_count, V_DEV, D)
    scale_blocks = logit_scale.reshape(block_count, V_DEV)
    block_ids = jnp.arange(block_count, dtype=jnp.int32)

    def advance(running, block_item):
        peaks, totals, picked = running
        block_index, block_rows, block_scale = block_item
        row_gain = block_scale * lax.rsqrt(lax.optimization_barrier(jnp.sum(jnp.square(block_rows.astype(jnp.float32)), axis=1)) + epsilon)
        logits = jnp.dot(hidden_unit, block_rows.T, preferred_element_type=jnp.float32) * row_gain[None, :]
        new_peaks = jnp.maximum(peaks, lax.optimization_barrier(jnp.max(logits, axis=1)))
        totals = totals * jnp.exp(peaks - new_peaks) + lax.optimization_barrier(jnp.sum(jnp.exp(logits - new_peaks[:, None]), axis=1))
        columns = block_index * V_DEV + jnp.arange(V_DEV, dtype=jnp.int32)
        picked = picked + lax.optimization_barrier(jnp.sum(jnp.where(columns[None, :] == targets[:, None], logits, jnp.float32(0.0)), axis=1))
        return ((new_peaks, totals, picked), None)
    start_state = (jnp.full((TOKENS,), -jnp.inf, jnp.float32), jnp.zeros((TOKENS,), jnp.float32), jnp.zeros((TOKENS,), jnp.float32))
    final_state, unused = lax.scan(advance, start_state, (block_ids, embed_blocks, scale_blocks))
    peaks, totals, picked = final_state
    token_loss = peaks + jnp.log(totals) - picked
    mean_loss = jnp.sum(token_loss) / TOKENS
    return (token_loss, mean_loss)
```

```python
import functools

import jax
import jax.numpy as jnp
from jax import lax
from jax.experimental import pallas as pl
from jax.experimental.pallas import tpu as pltpu
from jax.sharding import PartitionSpec as P

epsilon = 1e-06
NX, NZ, NC, NY = 4, 8, 2, 4
D = 4096
CA = 1024
CB = D - CA
CT = 128
ROWS = 16
HALF = NZ * ROWS
BLOCK = 256
f32, bf16 = jnp.float32, jnp.bfloat16
VMEM = pl.BlockSpec(memory_space=pltpu.VMEM)


def index_of(x, z, core):
    return ((x % NX) * NZ + z % NZ) * NC + core


def shift(array, dx, dz, flip=0):
    pairs = [
        (index_of(x, z, c), index_of(x + dx, z + dz, c ^ flip))
        for x in range(NX)
        for z in range(NZ)
        for c in range(NC)
    ]
    return lax.ppermute(array, "vocab", pairs)


def call(kernel, out_shape, name, limit, scratch=(), cost=None):
    return lambda *args: pl.pallas_call(
        kernel,
        out_shape=out_shape,
        in_specs=[VMEM] * len(args),
        out_specs=jax.tree.map(lambda _: VMEM, out_shape),
        scratch_shapes=list(scratch),
        compiler_params=pltpu.CompilerParams(vmem_limit_bytes=limit),
        cost_estimate=cost,
        name=name,
    )(*args)


def unit_kernel(hidden_ref, target_ref, a_ref, b_ref):
    wide = hidden_ref[...].astype(f32)
    unit = wide * lax.rsqrt(jnp.sum(wide * wide, axis=1, keepdims=True) + epsilon)
    unit = unit.astype(bf16)
    a_ref[...] = unit[:, :CA]
    b_ref[:, :CB] = unit[:, CA:]
    target = target_ref[...]
    high, low = target // 256, target % 256
    lane = lax.broadcasted_iota(jnp.int32, (ROWS, CT), 1)
    coded = jnp.where(lane == 0, high, jnp.where(lane == 1, low, 0))
    b_ref[:, CB:] = coded.astype(f32).astype(bf16)


def gain_kernel(embedding_ref, scale_ref, gain_ref):
    rows = embedding_ref.shape[0]

    def step(k, carry):
        part = pl.ds(pl.multiple_of(k * 64, 64), 64)
        total = jnp.zeros((64, 128), f32)
        for j in range(D // 128):
            piece = embedding_ref[part, j * 128 : (j + 1) * 128].astype(f32)
            total += piece * piece
        norm = lax.rsqrt(jnp.sum(total, axis=1, keepdims=True) + epsilon)
        gain_ref[part, :] = jnp.broadcast_to(norm * scale_ref[part, :], (64, 128))
        return carry

    lax.fori_loop(0, rows // 64, step, 0)


def place(index):
    core = index % NC
    z = (index // NC) % NZ
    return index // (NC * NZ), z, core


def statistics(blocks, tokens, target, gains, tables, logits, base):
    rows = tables[0].shape[0]
    per = rows // BLOCK
    peak = jnp.full((8, 256), -jnp.inf, f32)
    picked = jnp.zeros((8, 256), f32)
    for side in range(2):
        table, gain = tables[side], gains[side]

        def step(k, carry, table=table, gain=gain, side=side):
            peak, picked = carry
            part = pl.ds(pl.multiple_of(k * BLOCK, BLOCK), BLOCK)
            value = lax.dot_general(
                table[part, :], tokens[...], (((1,), (1,)), ((), ())), preferred_element_type=f32
            )
            factor = gain[part, :]
            value = value * jnp.concatenate([factor, factor], axis=1)
            whole = pl.ds(pl.multiple_of(side * rows + k * BLOCK, BLOCK), BLOCK)
            logits[whole, :] = value
            row = lax.broadcasted_iota(jnp.int32, (BLOCK, 256), 0) + (base[side] + k * BLOCK)
            chosen = jnp.where(row == target, value, 0.0)
            peak = jnp.maximum(peak, jnp.max(value.reshape(BLOCK // 8, 8, 256), axis=0))
            picked = picked + jnp.sum(chosen.reshape(BLOCK // 8, 8, 256), axis=0)
            return peak, picked

        peak, picked = lax.fori_loop(0, per, step, (peak, picked))
    peak = jnp.max(peak, axis=0, keepdims=True)

    def add(k, total):
        part = pl.ds(pl.multiple_of(k * BLOCK, BLOCK), BLOCK)
        term = jnp.exp(logits[part, :] - peak)
        return total + jnp.sum(term.reshape(BLOCK // 8, 8, 256), axis=0)

    total = lax.fori_loop(0, 2 * per, add, jnp.zeros((8, 256), f32))
    total = jnp.sum(total, axis=0, keepdims=True)
    return peak + jnp.log(total), jnp.sum(picked, axis=0, keepdims=True)


def head_kernel(a_spots, b_spots, last, n_a, n_b, *refs):
    own_table, swapped_table, own_gain, swapped_gain = refs[:4]
    a_refs = refs[4 : 4 + n_a]
    b_refs = refs[4 + n_a : 4 + n_a + n_b]
    rest = refs[4 + n_a + n_b :]
    if last:
        first_ref, *rest = rest
    out_ref, tokens, coded, logits = rest
    index = lax.axis_index("vocab")
    x, z, core = place(index)
    for buffer, row, half, dz in a_spots:
        at = pl.ds(pl.multiple_of(half * HALF + lax.rem(z + dz + NZ, NZ) * ROWS, ROWS), ROWS)
        tokens[at, :CA] = a_refs[buffer][row : row + ROWS, :]
    for buffer, row, half, dz in b_spots:
        at = pl.ds(pl.multiple_of(half * HALF + lax.rem(z + dz + NZ, NZ) * ROWS, ROWS), ROWS)
        tokens[at, CA:] = b_refs[buffer][row : row + ROWS, :CB]
        coded[at, :] = b_refs[buffer][row : row + ROWS, CB:].astype(f32)
    code = coded[...].T
    target = (code[0:1, :] * 256.0 + code[1:2, :]).astype(jnp.int32)
    rows = own_table.shape[0]
    base = (index * rows, (index + 1 - 2 * core) * rows)
    log_sum, picked = statistics(
        BLOCK, tokens, target, (own_gain, swapped_gain), (own_table, swapped_table), logits, base
    )
    row = lax.broadcasted_iota(jnp.int32, (8, 128), 0)

    def laid(sides, pair):
        both = jnp.zeros((8, 128), f32)
        for half in range(2):
            xs = lax.rem(x + pair[half] + NX, NX)
            lanes = slice(half * 128, half * 128 + 128)
            both = jnp.where(row == xs, sides[0][:, lanes], both)
            both = jnp.where(row == xs + NX, sides[1][:, lanes], both)
        return both

    if not last:
        out_ref[...] = laid((log_sum, picked), (-1, 1))
        return
    both = laid((log_sum, picked), (0, 2)) + first_ref[...]
    out_ref[...] = jnp.broadcast_to(both[None], out_ref.shape)


def close_kernel(pieces_ref, loss_ref, sum_ref):
    log_sum = pieces_ref[:, :NX, :]
    peak = jnp.max(log_sum, axis=0)
    total = jnp.sum(jnp.exp(log_sum - peak[None]), axis=0)
    loss = peak + jnp.log(total) - jnp.sum(pieces_ref[:, NX:, :], axis=0)
    loss_ref[...] = loss
    summed = jnp.sum(jnp.sum(loss, axis=0, keepdims=True), axis=1, keepdims=True)
    sum_ref[...] = jnp.broadcast_to(summed[None], sum_ref.shape)


def on_device(hidden, embedding, logit_scale, targets):
    rows = embedding.shape[0]
    index = lax.axis_index("vocab")
    x, z, core = place(index)
    a, b = call(
        unit_kernel,
        (
            jax.ShapeDtypeStruct((ROWS, CA), bf16),
            jax.ShapeDtypeStruct((ROWS, CB + CT), bf16),
        ),
        "unit",
        8 << 20,
    )(hidden, targets.reshape(ROWS, 1))
    swapped = shift(embedding, 0, 0, 1)
    swapped_scale = shift(logit_scale.reshape(8, 128), 0, 0, 1).reshape(rows, 1)
    gain = call(
        gain_kernel,
        jax.ShapeDtypeStruct((rows, 128), f32),
        "gain",
        24 << 20,
        cost=pl.CostEstimate(flops=4 * rows * D, bytes_accessed=2 * rows * D, transcendentals=0),
    )
    own_gain = gain(embedding, logit_scale.reshape(rows, 1))
    swapped_gain = gain(swapped, swapped_scale)

    a_left, a_right, a_far = shift(a, 1, 0), shift(a, -1, 0), shift(a, 2, 0)
    b1, c1, b2, c2 = shift(b, 0, 1), shift(b, 0, -1), shift(b, 0, 2), shift(b, 0, -2)
    b_left, b_right = shift(b, 1, 0), shift(b, -1, 0)
    line = jnp.concatenate([a_left, a_right, a, a_far])
    p1, m1 = shift(line, 0, 1), shift(line, 0, -1)
    near = jnp.concatenate([b1, c1, b2, c2])
    q1, n1 = shift(near, 1, 0), shift(near, -1, 0)
    p2, m2 = shift(line, 0, 2), shift(line, 0, -2)
    b3, c3, b4 = shift(b2, 0, 1), shift(c2, 0, -1), shift(b2, 0, 2)
    p3, m3, p4 = shift(p2, 0, 1), shift(m2, 0, -1), shift(p2, 0, 2)
    apart = jnp.concatenate([b3, c3, b4])
    q2, n2 = shift(apart, 1, 0), shift(apart, -1, 0)
    q3 = shift(q1, 1, 0)
    n3 = shift(jnp.concatenate([b_right, n2]), -1, 0)

    lines = (line, p1, m1, p2, m2, p3, m3, p4)
    line_dz = (0, -1, 1, -2, 2, -3, 3, -4)
    near_dz, apart_dz = (-1, 1, -2, 2), (-3, 3, -4)

    def spots(buffer, half, offsets):
        return [(buffer, k * ROWS, half, dz) for k, dz in enumerate(offsets)]

    cost = pl.CostEstimate(
        flops=2 * 2 * rows * D * 256, bytes_accessed=16 * rows * D, transcendentals=0
    )
    scratch = (
        pltpu.VMEM((256, D), bf16),
        pltpu.VMEM((256, CT), f32),
        pltpu.VMEM((2 * rows, 256), f32),
    )
    limit = 32 << 20
    a_spots = [(k, half * ROWS, half, dz) for k, dz in enumerate(line_dz) for half in (0, 1)]
    sides = (b_left, q1, q2, b_right, n1, n2)
    b_spots = []
    for half in (0, 1):
        b_spots += spots(3 * half, half, (0,))
        b_spots += spots(3 * half + 1, half, near_dz)
        b_spots += spots(3 * half + 2, half, apart_dz)
    tables = (embedding, swapped, own_gain, swapped_gain)
    first = call(
        functools.partial(head_kernel, a_spots, b_spots, False, 8, 6),
        jax.ShapeDtypeStruct((8, 128), f32),
        "head_sides",
        limit,
        scratch,
        cost,
    )(*tables, *lines, *sides)
    a_spots = [
        (k, (2 + half) * ROWS, half, dz) for k, dz in enumerate(line_dz) for half in (0, 1)
    ]
    columns = (b, near, apart, q3, n3)
    b_spots = spots(0, 0, (0,)) + spots(1, 0, near_dz) + spots(2, 0, apart_dz)
    b_spots += spots(3, 1, near_dz) + spots(4, 1, (0,) + apart_dz)
    pieces = call(
        functools.partial(head_kernel, a_spots, b_spots, True, 8, 5),
        jax.ShapeDtypeStruct((NX * NZ, 8, 128), f32),
        "head_column",
        limit,
        scratch,
        cost,
    )(*tables, *lines, *columns, first)

    same_core = [[v for v in range(NX * NZ * NC) if v % NC == c] for c in range(NC)]
    pieces = lax.all_to_all(
        pieces, "vocab", 0, 0, tiled=True, axis_index_groups=same_core
    )
    loss, summed = call(
        close_kernel,
        (jax.ShapeDtypeStruct((NX, 128), f32), jax.ShapeDtypeStruct((NY * NC, 1, 128), f32)),
        "close",
        8 << 20,
    )(pieces)
    groups = [
        [(v + c) * NY + s for c in range(NC) for s in range(NY)]
        for v in range(0, NX * NZ * NC, NC)
    ]
    summed = lax.all_to_all(
        summed, ("vocab", "seq"), 0, 0, tiled=True, axis_index_groups=groups
    )
    mean_loss = jnp.sum(summed[:, 0, 0]) / (NX * NZ * NC * NY * ROWS)
    own_loss = lax.dynamic_slice(loss, (x, z * ROWS), (1, ROWS)).reshape(ROWS)
    return own_loss, mean_loss


def solution(mesh):
    in_specs = (P(("vocab", "seq"), None), P("vocab", None), P("vocab"), P(("vocab", "seq")))
    out_specs = (P(("vocab", "seq")), P())
    return jax.shard_map(
        on_device, mesh=mesh, in_specs=in_specs, out_specs=out_specs, check_vma=False
    )
```

```python
import functools

import jax
import jax.numpy as jnp
from jax import lax
from jax.experimental import pallas as pl
from jax.experimental.pallas import tpu as pltpu
from jax.sharding import PartitionSpec as P

epsilon = 1e-06
NX, NZ, NC, NY = 4, 8, 2, 4
D = 4096
CA = 1024
CB = D - CA
CT = 128
ROWS = 16
HALF = NZ * ROWS
BLOCK = 256
f32, bf16 = jnp.float32, jnp.bfloat16
VMEM = pl.BlockSpec(memory_space=pltpu.VMEM)


def index_of(x, z, core):
    return ((x % NX) * NZ + z % NZ) * NC + core


def shift(array, dx, dz, flip=0):
    pairs = [
        (index_of(x, z, c), index_of(x + dx, z + dz, c ^ flip))
        for x in range(NX)
        for z in range(NZ)
        for c in range(NC)
    ]
    return lax.ppermute(array, "vocab", pairs)


def call(kernel, out_shape, name, limit, scratch=(), cost=None, specs=None):
    return lambda *args: pl.pallas_call(
        kernel,
        out_shape=out_shape,
        in_specs=specs or [VMEM] * len(args),
        out_specs=jax.tree.map(lambda _: VMEM, out_shape),
        scratch_shapes=list(scratch),
        compiler_params=pltpu.CompilerParams(vmem_limit_bytes=limit),
        cost_estimate=cost,
        name=name,
    )(*args)


def unit_kernel(hidden_ref, target_ref, unit_ref, a_ref, b_ref):
    wide = hidden_ref[...].astype(f32)
    unit = wide * lax.rsqrt(jnp.sum(wide * wide, axis=1, keepdims=True) + epsilon)
    unit = unit.astype(bf16)
    row = lax.broadcasted_iota(jnp.int32, (ROWS, ROWS), 0)
    column = lax.broadcasted_iota(jnp.int32, (ROWS, ROWS), 1)
    target = jnp.where(row == column, jnp.broadcast_to(target_ref[...], (ROWS, ROWS)), 0)
    high = jnp.sum((target // 256).astype(f32), axis=1, keepdims=True)
    low = jnp.sum((target % 256).astype(f32), axis=1, keepdims=True)
    lane = lax.broadcasted_iota(jnp.int32, (ROWS, CT), 1)
    coded = jnp.where(lane == 0, high, jnp.where(lane == 1, low, 0.0)).astype(bf16)
    unit_ref[:, :D] = unit
    unit_ref[:, D:] = coded
    a_ref[...] = unit[:, :CA]
    b_ref[:, :CB] = unit[:, CA:]
    b_ref[:, CB:] = coded


def table_kernel(embedding_ref, scale_ref, table_ref, gain_ref, arrived):
    steps = embedding_ref.shape[0] // 128

    def copy(k):
        part = pl.ds(pl.multiple_of(k * 128, 128), 128)
        return pltpu.make_async_copy(embedding_ref.at[part], table_ref.at[part], arrived.at[k])

    for k in range(steps):
        copy(k).start()

    def step(k, carry):
        copy(k).wait()
        part = pl.ds(pl.multiple_of(k * 128, 128), 128)
        total = jnp.zeros((128, 128), f32)
        for j in range(D // 128):
            piece = table_ref[part, j * 128 : (j + 1) * 128].astype(f32)
            total += piece * piece
        norm = lax.rsqrt(jnp.sum(total, axis=1, keepdims=True) + epsilon)
        scale = jnp.broadcast_to(scale_ref[pl.ds(k, 1), :], (128, 128)).T
        gain_ref[part, :] = norm * scale
        return carry

    lax.fori_loop(0, steps, step, 0)


def place(index):
    core = index % NC
    z = (index // NC) % NZ
    return index // (NC * NZ), z, core


def head_kernel(a_spots, b_spots, last, counts, *refs):
    own_table, swapped_ref, own_gain, swapped_gain = refs[:4]
    n_a, n_b = counts
    a_refs = refs[4 : 4 + n_a]
    b_refs = refs[4 + n_a : 4 + n_a + n_b]
    rest = refs[4 + n_a + n_b :]
    if last:
        first_ref, *rest = rest
    out_ref, tokens, coded, logits, swapped_table, arrived = rest
    copy = pltpu.make_async_copy(swapped_ref, swapped_table, arrived)
    copy.start()
    index = lax.axis_index("vocab")
    x, z, core = place(index)

    def spot(half, dz):
        return pl.ds(pl.multiple_of(half * HALF + lax.rem(z + dz + NZ, NZ) * ROWS, ROWS), ROWS)

    for buffer, row, column, half, dz in a_spots:
        tokens[spot(half, dz), :CA] = a_refs[buffer][row : row + ROWS, column : column + CA]
    for buffer, row, column, half, dz in b_spots:
        ref = b_refs[buffer]
        tokens[spot(half, dz), CA:] = ref[row : row + ROWS, column : column + CB]
        coded[spot(half, dz), :] = ref[row : row + ROWS, column + CB : column + CB + CT].astype(f32)
    code = coded[...].T
    target = (code[0:1, :] * 256.0 + code[1:2, :]).astype(jnp.int32)
    rows = own_table.shape[0]
    peak = jnp.full((8, 256), -jnp.inf, f32)
    picked = jnp.zeros((8, 256), f32)
    for side in range(2):
        if side:
            copy.wait()
        table, gain = ((own_table, own_gain), (swapped_table, swapped_gain))[side]
        base = (index, index + 1 - 2 * core)[side] * rows
        value = lax.dot_general(
            table[...], tokens[...], (((1,), (1,)), ((), ())), preferred_element_type=f32
        )
        factor = gain[...]
        value = value * jnp.concatenate([factor, factor], axis=1)
        logits[side * rows : (side + 1) * rows, :] = value
        row = lax.broadcasted_iota(jnp.int32, (rows, 256), 0) + base
        chosen = jnp.where(row == target, value, 0.0)
        peak = jnp.maximum(peak, jnp.max(value.reshape(rows // 8, 8, 256), axis=0))
        picked = picked + jnp.sum(chosen.reshape(rows // 8, 8, 256), axis=0)
    peak = jnp.max(peak, axis=0, keepdims=True)

    def add(k, total):
        part = pl.ds(pl.multiple_of(k * BLOCK, BLOCK), BLOCK)
        term = jnp.exp(logits[part, :] - peak)
        return total + jnp.sum(term.reshape(BLOCK // 8, 8, 256), axis=0)

    total = lax.fori_loop(0, 2 * rows // BLOCK, add, jnp.zeros((8, 256), f32))
    log_sum = peak + jnp.log(jnp.sum(total, axis=0, keepdims=True))
    picked = jnp.sum(picked, axis=0, keepdims=True)
    row = lax.broadcasted_iota(jnp.int32, (8, 128), 0)
    both = first_ref[...] if last else jnp.zeros((8, 128), f32)
    for half, dx in enumerate((0, 2) if last else (-1, 1)):
        xs = lax.rem(x + dx + NX, NX)
        lanes = slice(half * 128, half * 128 + 128)
        both = jnp.where(row == xs, log_sum[:, lanes], both)
        both = jnp.where(row == xs + NX, picked[:, lanes], both)
    out_ref[...] = both


def joined(pieces):
    peak = functools.reduce(jnp.maximum, pieces)
    total = functools.reduce(jnp.add, [jnp.exp(piece - peak) for piece in pieces])
    row = lax.broadcasted_iota(jnp.int32, (8, 128), 0)
    return jnp.where(row < NX, peak + jnp.log(total), functools.reduce(jnp.add, pieces))


def join_kernel(*refs):
    refs[-1][...] = joined([ref[...] for ref in refs[:-1]])


def close_kernel(own_ref, beside_ref, other_ref, across_ref, loss_ref, sum_ref):
    own = joined([own_ref[...], beside_ref[...]])
    other = joined([other_ref[...], across_ref[...]])
    loss = own[:NX, :] - own[NX:, :]
    loss_ref[...] = loss
    both = loss + (other[:NX, :] - other[NX:, :])
    summed = jnp.sum(jnp.sum(both, axis=0, keepdims=True), axis=1, keepdims=True)
    sum_ref[...] = jnp.broadcast_to(summed, sum_ref.shape)


def permuted(array, move):
    pairs = [
        (index_of(x, z, c), index_of(*move(x, z, c)))
        for x in range(NX)
        for z in range(NZ)
        for c in range(NC)
    ]
    return lax.ppermute(array, "vocab", pairs)


def on_device(hidden, embedding, logit_scale, targets):
    rows = embedding.shape[0]
    index = lax.axis_index("vocab")
    x, z, core = place(index)
    swapped = shift(embedding, 0, 0, 1)
    unit, a, b = call(
        unit_kernel,
        (
            jax.ShapeDtypeStruct((ROWS, D + CT), bf16),
            jax.ShapeDtypeStruct((ROWS, CA), bf16),
            jax.ShapeDtypeStruct((ROWS, CB + CT), bf16),
        ),
        "unit",
        8 << 20,
    )(hidden, targets.reshape(1, ROWS))
    any_space = pl.BlockSpec(memory_space=pltpu.HBM)
    table, own_gain = call(
        table_kernel,
        (pltpu.VMEM((rows, D), bf16), jax.ShapeDtypeStruct((rows, 128), f32)),
        "table",
        32 << 20,
        (pltpu.SemaphoreType.DMA((rows // 128,)),),
        pl.CostEstimate(flops=16 * rows * D, bytes_accessed=4 * rows * D, transcendentals=0),
        [any_space, VMEM],
    )(embedding, logit_scale.reshape(rows // 128, 128))

    a_far = shift(a, 2, 0)
    left, right = shift(unit, 1, 0), shift(unit, -1, 0)
    b1, c1, b2, c2 = shift(b, 0, 1), shift(b, 0, -1), shift(b, 0, 2), shift(b, 0, -2)
    line = jnp.concatenate([left[:, :CA], right[:, :CA], a, a_far])
    line, table, own_gain = lax.optimization_barrier((line, table, own_gain))
    p1, m1 = shift(line, 0, 1), shift(line, 0, -1)
    near = jnp.concatenate([b1, c1, b2, c2])
    q1, n1 = shift(near, 1, 0), shift(near, -1, 0)
    p2, m2 = shift(line, 0, 2), shift(line, 0, -2)
    b3, c3, b4 = shift(b2, 0, 1), shift(c2, 0, -1), shift(b2, 0, 2)
    p3, m3, p4 = shift(p2, 0, 1), shift(m2, 0, -1), shift(p2, 0, 2)
    apart = jnp.concatenate([b3, c3, b4])
    q2, n2 = shift(apart, 1, 0), shift(apart, -1, 0)
    q3 = shift(q1, 1, 0)
    n3 = shift(jnp.concatenate([right[:, CA:], n2]), -1, 0)
    swapped_gain = shift(own_gain, 0, 0, 1)

    lines = (line, p1, m1, p2, m2, p3, m3, p4)
    line_dz = (0, -1, 1, -2, 2, -3, 3, -4)
    near_dz, apart_dz = (-1, 1, -2, 2), (-3, 3, -4)

    def spots(buffer, half, offsets, column=0):
        return [(buffer, k * ROWS, column, half, dz) for k, dz in enumerate(offsets)]

    cost = pl.CostEstimate(
        flops=2 * 2 * rows * D * 256, bytes_accessed=16 * rows * D, transcendentals=0
    )
    scratch = (
        pltpu.VMEM((256, D), bf16),
        pltpu.VMEM((256, CT), f32),
        pltpu.VMEM((2 * rows, 256), f32),
        pltpu.VMEM((rows, D), bf16),
        pltpu.SemaphoreType.DMA,
    )
    limit = 40 << 20
    tables = (table, swapped, own_gain, swapped_gain)

    def head(a_spots, b_spots, last, sources, name):
        count = len(tables) + len(lines) + len(sources)
        return call(
            functools.partial(
                head_kernel, a_spots, b_spots, last, (len(lines), len(sources) - last)
            ),
            jax.ShapeDtypeStruct((8, 128), f32),
            name,
            limit,
            scratch,
            cost,
            [any_space if k == 1 else VMEM for k in range(count)],
        )(*tables, *lines, *sources)

    a_spots = [(k, half * ROWS, 0, half, dz) for k, dz in enumerate(line_dz) for half in (0, 1)]
    b_spots = []
    for half in (0, 1):
        b_spots += spots(3 * half, half, (0,), CA)
        b_spots += spots(3 * half + 1, half, near_dz)
        b_spots += spots(3 * half + 2, half, apart_dz)
    first = head(a_spots, b_spots, False, (left, q1, q2, right, n1, n2), "head_sides")
    a_spots = [
        (k, (2 + half) * ROWS, 0, half, dz) for k, dz in enumerate(line_dz) for half in (0, 1)
    ]
    b_spots = spots(0, 0, (0,)) + spots(1, 0, near_dz) + spots(2, 0, apart_dz)
    b_spots += spots(3, 1, near_dz) + spots(4, 1, (0,) + apart_dz)
    mine = head(a_spots, b_spots, True, (b, near, apart, q3, n3, first), "head_column")

    piece = jax.ShapeDtypeStruct((8, 128), f32)
    mine = call(join_kernel, piece, "join_x", 4 << 20)(
        mine, *(shift(mine, d, 0) for d in (1, 2, 3))
    )
    mine = call(join_kernel, piece, "join_z", 4 << 20)(
        mine, *(shift(mine, 0, d) for d in (2, 4, 6))
    )
    beside = permuted(mine, lambda x, z, c: (x, z ^ 1, c))
    other = permuted(mine, lambda x, z, c: (x, z, c ^ 1))
    across = permuted(mine, lambda x, z, c: (x, z ^ 1, c ^ 1))
    loss, summed = call(
        close_kernel,
        (jax.ShapeDtypeStruct((NX, 128), f32), jax.ShapeDtypeStruct((1, 128), f32)),
        "close",
        4 << 20,
    )(mine, beside, other, across)
    far = [
        lax.ppermute(summed, "seq", [(s, (s + d) % NY) for s in range(NY)]) for d in (1, 2, 3)
    ]
    own_loss = lax.dynamic_slice(loss, (x, z * ROWS), (1, ROWS)).reshape(ROWS)
    mean_loss = (summed + far[0] + far[1] + far[2])[0, 0] / (NX * NZ * NC * NY * ROWS)
    return own_loss, mean_loss


def solution(mesh):
    in_specs = (P(("vocab", "seq"), None), P("vocab", None), P("vocab"), P(("vocab", "seq")))
    out_specs = (P(("vocab", "seq")), P())
    return jax.shard_map(
        on_device, mesh=mesh, in_specs=in_specs, out_specs=out_specs, check_vma=False
    )
```

```python
import functools

import jax
import jax.numpy as jnp
from jax import lax
from jax.experimental import pallas as pl
from jax.experimental.pallas import tpu as pltpu
from jax.sharding import PartitionSpec as P

epsilon = 1e-06
NX, NZ, NC, NY = 4, 8, 2, 4
D = 4096
CA = 1024
CB = D - CA
CT = 128
ROWS = 16
HALF = NZ * ROWS
BLOCK = 512
f32, bf16 = jnp.float32, jnp.bfloat16
VMEM = pl.BlockSpec(memory_space=pltpu.VMEM)


def index_of(x, z, core):
    return ((x % NX) * NZ + z % NZ) * NC + core


def shift(array, dx, dz, flip=0):
    pairs = [
        (index_of(x, z, c), index_of(x + dx, z + dz, c ^ flip))
        for x in range(NX)
        for z in range(NZ)
        for c in range(NC)
    ]
    return lax.ppermute(array, "vocab", pairs)


def call(kernel, out_shape, name, limit, scratch=(), cost=None, specs=None):
    return lambda *args: pl.pallas_call(
        kernel,
        out_shape=out_shape,
        in_specs=specs or [VMEM] * len(args),
        out_specs=jax.tree.map(lambda _: VMEM, out_shape),
        scratch_shapes=list(scratch),
        compiler_params=pltpu.CompilerParams(vmem_limit_bytes=limit),
        cost_estimate=cost,
        name=name,
    )(*args)


def unit_kernel(hidden_hbm, target_hbm, unit_ref, a_ref, b_ref, hidden_ref, target_ref, arrived):
    copies = (
        pltpu.make_async_copy(hidden_hbm, hidden_ref, arrived.at[0]),
        pltpu.make_async_copy(target_hbm, target_ref, arrived.at[1]),
    )
    for copy in copies:
        copy.start()
    for copy in copies:
        copy.wait()
    wide = hidden_ref[...].astype(f32)
    unit = wide * lax.rsqrt(jnp.sum(wide * wide, axis=1, keepdims=True) + epsilon)
    unit = unit.astype(bf16)
    row = lax.broadcasted_iota(jnp.int32, (ROWS, ROWS), 0)
    column = lax.broadcasted_iota(jnp.int32, (ROWS, ROWS), 1)
    target = jnp.where(row == column, jnp.broadcast_to(target_ref[...], (ROWS, ROWS)), 0)
    high = jnp.sum((target // 256).astype(f32), axis=1, keepdims=True)
    low = jnp.sum((target % 256).astype(f32), axis=1, keepdims=True)
    lane = lax.broadcasted_iota(jnp.int32, (ROWS, CT), 1)
    coded = jnp.where(lane == 0, high, jnp.where(lane == 1, low, 0.0)).astype(bf16)
    unit_ref[:, :D] = unit
    unit_ref[:, D:] = coded
    a_ref[...] = unit[:, :CA]
    b_ref[:, :CB] = unit[:, CA:]
    b_ref[:, CB:] = coded


def gain_kernel(embedding_ref, scale_hbm, gain_ref, table_ref, scale_ref, arrived):
    steps = embedding_ref.shape[0] // 128

    def copy(k):
        part = pl.ds(pl.multiple_of(k * 128, 128), 128)
        return pltpu.make_async_copy(embedding_ref.at[part], table_ref.at[part], arrived.at[k])

    scales = pltpu.make_async_copy(scale_hbm, scale_ref, arrived.at[steps])
    scales.start()
    for k in range(steps):
        copy(k).start()
    scales.wait()

    def step(k, carry):
        copy(k).wait()
        part = pl.ds(pl.multiple_of(k * 128, 128), 128)
        total = jnp.zeros((128, 128), f32)
        for j in range(D // 128):
            piece = table_ref[part, j * 128 : (j + 1) * 128].astype(f32)
            total += piece * piece
        norm = lax.rsqrt(jnp.sum(total, axis=1, keepdims=True) + epsilon)
        scale = jnp.broadcast_to(scale_ref[pl.ds(k, 1), :], (128, 128)).T
        gain_ref[part, :] = norm * scale
        return carry

    lax.fori_loop(0, steps, step, 0)


def place(index):
    core = index % NC
    z = (index // NC) % NZ
    return index // (NC * NZ), z, core


def head_kernel(a_spots, b_spots, last, counts, *refs):
    n_a, n_b = counts
    if last:
        tables, own_gain, swapped_gain, first_ref, *rest = refs
    else:
        own_ref, swapped_ref, own_gain, swapped_gain, *rest = refs
    a_refs, b_refs, rest = rest[:n_a], rest[n_a : n_a + n_b], rest[n_a + n_b :]
    if last:
        out_ref, tokens, coded, gains, logits = rest
    else:
        out_ref, tables, tokens, coded, gains, logits, arrived = rest
    rows = tables.shape[0] // 2
    blocks = 2 * rows // BLOCK

    if not last:
        copies = []
        for k in range(blocks):
            source = (own_ref, swapped_ref)[k * BLOCK // rows]
            at = pl.ds(k * BLOCK % rows, BLOCK)
            copies.append(
                pltpu.make_async_copy(source.at[at], tables.at[pl.ds(k * BLOCK, BLOCK)], arrived.at[k])
            )
            copies[k].start()
    gains[:rows, :] = own_gain[...]
    gains[rows:, :] = swapped_gain[...]
    index = lax.axis_index("vocab")
    x, z, core = place(index)

    def spot(half, dz):
        return pl.ds(pl.multiple_of(half * HALF + lax.rem(z + dz + NZ, NZ) * ROWS, ROWS), ROWS)

    for buffer, row, column, half, dz in a_spots:
        tokens[spot(half, dz), :CA] = a_refs[buffer][row : row + ROWS, column : column + CA]
    for buffer, row, column, half, dz in b_spots:
        ref = b_refs[buffer]
        tokens[spot(half, dz), CA:] = ref[row : row + ROWS, column : column + CB]
        coded[spot(half, dz), :] = ref[row : row + ROWS, column + CB : column + CB + CT].astype(f32)
    code = coded[...].T
    target = (code[0:1, :] * 256.0 + code[1:2, :]).astype(jnp.int32)
    own_base, swapped_base = index * rows, (index - 2 * core) * rows

    def step(k, carry):
        peak, picked = carry
        part = pl.ds(pl.multiple_of(k * BLOCK, BLOCK), BLOCK)
        if not last:
            pltpu.make_async_copy(own_ref.at[pl.ds(0, BLOCK)], tables.at[part], arrived.at[k]).wait()
        value = lax.dot_general(
            tables[part, :], tokens[...], (((1,), (1,)), ((), ())), preferred_element_type=f32
        )
        factor = gains[part, :]
        value = value * jnp.concatenate([factor, factor], axis=1)
        logits[part, :] = value
        base = jnp.where(k * BLOCK < rows, own_base, swapped_base) + k * BLOCK
        row = lax.broadcasted_iota(jnp.int32, (BLOCK, 256), 0)
        chosen = jnp.where(row == target - base, value, 0.0)
        peak = jnp.maximum(peak, jnp.max(value.reshape(BLOCK // 8, 8, 256), axis=0))
        picked = picked + jnp.sum(chosen.reshape(BLOCK // 8, 8, 256), axis=0)
        return peak, picked

    peak, picked = lax.fori_loop(
        0, blocks, step, (jnp.full((8, 256), -jnp.inf, f32), jnp.zeros((8, 256), f32))
    )
    peak = jnp.max(peak, axis=0, keepdims=True)

    def add(k, total):
        part = pl.ds(pl.multiple_of(k * 256, 256), 256)
        term = jnp.exp(logits[part, :] - peak)
        return total + jnp.sum(term.reshape(32, 8, 256), axis=0)

    total = lax.fori_loop(0, 2 * rows // 256, add, jnp.zeros((8, 256), f32))
    log_sum = peak + jnp.log(jnp.sum(total, axis=0, keepdims=True))
    picked = jnp.sum(picked, axis=0, keepdims=True)
    row = lax.broadcasted_iota(jnp.int32, (8, 128), 0)
    both = first_ref[...] if last else jnp.zeros((8, 128), f32)
    for half, dx in enumerate((0, 2) if last else (-1, 1)):
        xs = lax.rem(x + dx + NX, NX)
        lanes = slice(half * 128, half * 128 + 128)
        both = jnp.where(row == xs, log_sum[:, lanes], both)
        both = jnp.where(row == xs + NX, picked[:, lanes], both)
    out_ref[...] = both


def joined(pieces):
    peak = functools.reduce(jnp.maximum, pieces)
    total = functools.reduce(jnp.add, [jnp.exp(piece - peak) for piece in pieces])
    row = lax.broadcasted_iota(jnp.int32, (8, 128), 0)
    return jnp.where(row < NX, peak + jnp.log(total), functools.reduce(jnp.add, pieces))


def join_kernel(*refs):
    refs[-1][...] = joined([ref[...] for ref in refs[:-1]])


def close_kernel(own_ref, other_ref, loss_ref, sum_ref):
    own, other = own_ref[...], other_ref[...]
    loss = own[:NX, :] - own[NX:, :]
    loss_ref[...] = loss
    both = loss + (other[:NX, :] - other[NX:, :])
    summed = jnp.sum(jnp.sum(both, axis=0, keepdims=True), axis=1, keepdims=True)
    sum_ref[...] = jnp.broadcast_to(summed, sum_ref.shape)


def permuted(array, move):
    pairs = [
        (index_of(x, z, c), index_of(*move(x, z, c)))
        for x in range(NX)
        for z in range(NZ)
        for c in range(NC)
    ]
    return lax.ppermute(array, "vocab", pairs)


def on_device(hidden, embedding, logit_scale, targets):
    rows = embedding.shape[0]
    index = lax.axis_index("vocab")
    x, z, core = place(index)
    swapped = shift(embedding, 0, 0, 1)
    any_space = pl.BlockSpec(memory_space=pltpu.HBM)
    unit, a, b = call(
        unit_kernel,
        (
            jax.ShapeDtypeStruct((ROWS, D + CT), bf16),
            jax.ShapeDtypeStruct((ROWS, CA), bf16),
            jax.ShapeDtypeStruct((ROWS, CB + CT), bf16),
        ),
        "unit",
        60 << 20,
        (
            pltpu.VMEM((ROWS, D), bf16),
            pltpu.VMEM((1, ROWS), jnp.int32),
            pltpu.SemaphoreType.DMA((2,)),
        ),
        specs=[any_space, any_space],
    )(hidden, targets.reshape(1, ROWS))
    own_gain = call(
        gain_kernel,
        jax.ShapeDtypeStruct((rows, 128), f32),
        "gain",
        58 << 20,
        (
            pltpu.VMEM((rows, D), bf16),
            pltpu.VMEM((rows // 128, 128), f32),
            pltpu.SemaphoreType.DMA((rows // 128 + 1,)),
        ),
        pl.CostEstimate(flops=16 * rows * D, bytes_accessed=4 * rows * D, transcendentals=0),
        [any_space, any_space],
    )(embedding, logit_scale.reshape(rows // 128, 128))

    a_far = shift(a, 2, 0)
    left, right = shift(unit, 1, 0), shift(unit, -1, 0)
    b1, c1, b2, c2 = shift(b, 0, 1), shift(b, 0, -1), shift(b, 0, 2), shift(b, 0, -2)
    line = jnp.concatenate([left[:, :CA], right[:, :CA], a, a_far])
    line, own_gain = lax.optimization_barrier((line, own_gain))
    p1, m1 = shift(line, 0, 1), shift(line, 0, -1)
    near = jnp.concatenate([b1, c1, b2, c2])
    q1, n1 = shift(near, 1, 0), shift(near, -1, 0)
    p2, m2 = shift(line, 0, 2), shift(line, 0, -2)
    b3, c3, b4 = shift(b2, 0, 1), shift(c2, 0, -1), shift(b2, 0, 2)
    p3, m3, p4 = shift(p2, 0, 1), shift(m2, 0, -1), shift(p2, 0, 2)
    apart = jnp.concatenate([b3, c3, b4])
    q2, n2 = shift(apart, 1, 0), shift(apart, -1, 0)
    q3 = shift(q1, 1, 0)
    n3 = shift(jnp.concatenate([right[:, CA:], n2]), -1, 0)
    swapped_gain = shift(own_gain, 0, 0, 1)

    lines = (line, p1, m1, p2, m2, p3, m3, p4)
    line_dz = (0, -1, 1, -2, 2, -3, 3, -4)
    near_dz, apart_dz = (-1, 1, -2, 2), (-3, 3, -4)

    def spots(buffer, half, offsets, column=0):
        return [(buffer, k * ROWS, column, half, dz) for k, dz in enumerate(offsets)]

    cost = pl.CostEstimate(
        flops=2 * 2 * rows * D * 256, bytes_accessed=16 * rows * D, transcendentals=0
    )
    scratch = (
        pltpu.VMEM((256, D), bf16),
        pltpu.VMEM((256, CT), f32),
        pltpu.VMEM((2 * rows, 128), f32),
        pltpu.VMEM((2 * rows, 256), f32),
    )

    def head(a_spots, b_spots, given, sources, name, limit):
        last = name == "head_column"
        given = (
            (given[0], own_gain, swapped_gain, given[1]) if last else (*given, own_gain, swapped_gain)
        )
        piece = jax.ShapeDtypeStruct((8, 128), f32)
        return call(
            functools.partial(head_kernel, a_spots, b_spots, last, (len(lines), len(sources))),
            piece if last else (piece, pltpu.VMEM((2 * rows, D), bf16)),
            name,
            limit,
            scratch if last else (*scratch, pltpu.SemaphoreType.DMA((2 * rows // BLOCK,))),
            cost,
            [VMEM] * (len(given) + len(lines) + len(sources))
            if last
            else [any_space] * 2 + [VMEM] * (2 + len(lines) + len(sources)),
        )(*given, *lines, *sources)

    a_spots = [(k, half * ROWS, 0, half, dz) for k, dz in enumerate(line_dz) for half in (0, 1)]
    b_spots = []
    for half in (0, 1):
        b_spots += spots(3 * half, half, (0,), CA)
        b_spots += spots(3 * half + 1, half, near_dz)
        b_spots += spots(3 * half + 2, half, apart_dz)
    sides = (left, q1, q2, right, n1, n2)
    first, tables = head(a_spots, b_spots, (embedding, swapped), sides, "head_sides", 28 << 20)
    a_spots = [
        (k, (2 + half) * ROWS, 0, half, dz) for k, dz in enumerate(line_dz) for half in (0, 1)
    ]
    b_spots = spots(0, 0, (0,)) + spots(1, 0, near_dz) + spots(2, 0, apart_dz)
    b_spots += spots(3, 1, near_dz) + spots(4, 1, (0,) + apart_dz)
    columns = (b, near, apart, q3, n3)
    mine = head(a_spots, b_spots, (tables, first), columns, "head_column", 28 << 20)

    piece = jax.ShapeDtypeStruct((8, 128), f32)
    for k, move in enumerate(
        (
            lambda x, z, c: (x ^ 1, z, c),
            lambda x, z, c: (x + 2 * (x % 2) - 1, z, c),
            lambda x, z, c: (x, z ^ 1, c),
            lambda x, z, c: (x, z + 2 * (z % 2) - 1, c),
            lambda x, z, c: (x, z + 4, c),
        )
    ):
        mine = call(join_kernel, piece, f"join_{k}", 4 << 20)(mine, permuted(mine, move))
    other = permuted(mine, lambda x, z, c: (x, z, c ^ 1))
    loss, summed = call(
        close_kernel,
        (jax.ShapeDtypeStruct((NX, 128), f32), jax.ShapeDtypeStruct((1, 128), f32)),
        "close",
        4 << 20,
    )(mine, other)
    for step in ([1, 0, 3, 2], [3, 2, 1, 0]):
        summed = summed + lax.ppermute(summed, "seq", list(enumerate(step)))
    own_loss = lax.dynamic_slice(loss, (x, z * ROWS), (1, ROWS)).reshape(ROWS)
    mean_loss = summed[0, 0] / (NX * NZ * NC * NY * ROWS)
    return own_loss, mean_loss


def solution(mesh):
    in_specs = (P(("vocab", "seq"), None), P("vocab", None), P("vocab"), P(("vocab", "seq")))
    out_specs = (P(("vocab", "seq")), P())
    return jax.shard_map(
        on_device, mesh=mesh, in_specs=in_specs, out_specs=out_specs, check_vma=False
    )
```

```python
import functools

import jax
import jax.numpy as jnp
from jax import lax
from jax.experimental import pallas as pl
from jax.experimental.pallas import tpu as pltpu
from jax.sharding import PartitionSpec as P

epsilon = 1e-06
NX, NZ, NC, NY = 4, 8, 2, 4
D = 4096
CA = 1024
CB = D - CA
CT = 128
ROWS = 16
HALF = NZ * ROWS
BLOCK = 512
f32, bf16 = jnp.float32, jnp.bfloat16
VMEM = pl.BlockSpec(memory_space=pltpu.VMEM)


def index_of(x, z, core):
    return ((x % NX) * NZ + z % NZ) * NC + core


def shift(array, dx, dz, flip=0):
    pairs = [
        (index_of(x, z, c), index_of(x + dx, z + dz, c ^ flip))
        for x in range(NX)
        for z in range(NZ)
        for c in range(NC)
    ]
    return lax.ppermute(array, "vocab", pairs)


def call(kernel, out_shape, name, limit, scratch=(), cost=None, specs=None):
    return lambda *args: pl.pallas_call(
        kernel,
        out_shape=out_shape,
        in_specs=specs or [VMEM] * len(args),
        out_specs=jax.tree.map(lambda _: VMEM, out_shape),
        scratch_shapes=list(scratch),
        compiler_params=pltpu.CompilerParams(vmem_limit_bytes=limit),
        cost_estimate=cost,
        name=name,
    )(*args)


def unit_kernel(hidden_hbm, target_hbm, unit_ref, a_ref, b_ref, hidden_ref, target_ref, arrived):
    copies = (
        pltpu.make_async_copy(hidden_hbm, hidden_ref, arrived.at[0]),
        pltpu.make_async_copy(target_hbm, target_ref, arrived.at[1]),
    )
    for copy in copies:
        copy.start()
    for copy in copies:
        copy.wait()
    wide = hidden_ref[...].astype(f32)
    unit = wide * lax.rsqrt(jnp.sum(wide * wide, axis=1, keepdims=True) + epsilon)
    unit = unit.astype(bf16)
    row = lax.broadcasted_iota(jnp.int32, (ROWS, ROWS), 0)
    column = lax.broadcasted_iota(jnp.int32, (ROWS, ROWS), 1)
    target = jnp.where(row == column, jnp.broadcast_to(target_ref[...], (ROWS, ROWS)), 0)
    high = jnp.sum((target // 256).astype(f32), axis=1, keepdims=True)
    low = jnp.sum((target % 256).astype(f32), axis=1, keepdims=True)
    lane = lax.broadcasted_iota(jnp.int32, (ROWS, CT), 1)
    coded = jnp.where(lane == 0, high, jnp.where(lane == 1, low, 0.0)).astype(bf16)
    unit_ref[:, :D] = unit
    unit_ref[:, D:] = coded
    a_ref[...] = unit[:, :CA]
    b_ref[:, :CB] = unit[:, CA:]
    b_ref[:, CB:] = coded


def place(index):
    core = index % NC
    z = (index // NC) % NZ
    return index // (NC * NZ), z, core


def head_kernel(a_spots, b_spots, last, counts, *refs):
    n_a, n_b = counts
    if last:
        tables, gains, first_ref, *rest = refs
    else:
        own_ref, swapped_ref, scale_ref, swapped_scale, *rest = refs
    a_refs, b_refs, rest = rest[:n_a], rest[n_a : n_a + n_b], rest[n_a + n_b :]
    if last:
        out_ref, tokens, coded, logits = rest
    else:
        out_ref, tables, gains, tokens, coded, logits, scales, arrived = rest
    rows = tables.shape[0] // 2
    blocks = 2 * rows // BLOCK

    if not last:
        own_scale = pltpu.make_async_copy(scale_ref, scales.at[pl.ds(0, rows // 128)], arrived.at[blocks])
        own_scale.start()
        for k in range(blocks):
            source = (own_ref, swapped_ref)[k * BLOCK // rows]
            at = pl.ds(k * BLOCK % rows, BLOCK)
            pltpu.make_async_copy(
                source.at[at], tables.at[pl.ds(k * BLOCK, BLOCK)], arrived.at[k]
            ).start()
        scales[rows // 128 :, :] = swapped_scale[...]
        own_scale.wait()
    index = lax.axis_index("vocab")
    x, z, core = place(index)

    def spot(half, dz):
        return pl.ds(pl.multiple_of(half * HALF + lax.rem(z + dz + NZ, NZ) * ROWS, ROWS), ROWS)

    for buffer, row, column, half, dz in a_spots:
        tokens[spot(half, dz), :CA] = a_refs[buffer][row : row + ROWS, column : column + CA]
    for buffer, row, column, half, dz in b_spots:
        ref = b_refs[buffer]
        tokens[spot(half, dz), CA:] = ref[row : row + ROWS, column : column + CB]
        coded[spot(half, dz), :] = ref[row : row + ROWS, column + CB : column + CB + CT].astype(f32)
    code = coded[...].T
    target = (code[0:1, :] * 256.0 + code[1:2, :]).astype(jnp.int32)
    own_base, swapped_base = index * rows, (index - 2 * core) * rows

    def step(k, carry):
        peak, picked = carry
        part = pl.ds(pl.multiple_of(k * BLOCK, BLOCK), BLOCK)
        if not last:
            pltpu.make_async_copy(own_ref.at[pl.ds(0, BLOCK)], tables.at[part], arrived.at[k]).wait()
            for j in range(BLOCK // 128):
                some = pl.ds(pl.multiple_of(k * BLOCK + j * 128, 128), 128)
                total = jnp.zeros((128, 128), f32)
                for i in range(D // 128):
                    piece = tables[some, i * 128 : (i + 1) * 128].astype(f32)
                    total += piece * piece
                norm = lax.rsqrt(jnp.sum(total, axis=1, keepdims=True) + epsilon)
                scale = scales[pl.ds(k * (BLOCK // 128) + j, 1), :]
                gains[some, :] = norm * jnp.broadcast_to(scale, (128, 128)).T
        value = lax.dot_general(
            tables[part, :], tokens[...], (((1,), (1,)), ((), ())), preferred_element_type=f32
        )
        factor = gains[part, :]
        value = value * jnp.concatenate([factor, factor], axis=1)
        logits[part, :] = value
        base = jnp.where(k * BLOCK < rows, own_base, swapped_base) + k * BLOCK
        row = lax.broadcasted_iota(jnp.int32, (BLOCK, 256), 0)
        chosen = jnp.where(row == target - base, value, 0.0)
        peak = jnp.maximum(peak, jnp.max(value.reshape(BLOCK // 8, 8, 256), axis=0))
        picked = picked + jnp.sum(chosen.reshape(BLOCK // 8, 8, 256), axis=0)
        return peak, picked

    peak, picked = lax.fori_loop(
        0, blocks, step, (jnp.full((8, 256), -jnp.inf, f32), jnp.zeros((8, 256), f32))
    )
    peak = jnp.max(peak, axis=0, keepdims=True)

    def add(k, total):
        part = pl.ds(pl.multiple_of(k * 256, 256), 256)
        term = jnp.exp(logits[part, :] - peak)
        return total + jnp.sum(term.reshape(32, 8, 256), axis=0)

    total = lax.fori_loop(0, 2 * rows // 256, add, jnp.zeros((8, 256), f32))
    log_sum = peak + jnp.log(jnp.sum(total, axis=0, keepdims=True))
    picked = jnp.sum(picked, axis=0, keepdims=True)
    row = lax.broadcasted_iota(jnp.int32, (8, 128), 0)
    both = first_ref[...] if last else jnp.zeros((8, 128), f32)
    for half, dx in enumerate((0, 2) if last else (-1, 1)):
        xs = lax.rem(x + dx + NX, NX)
        lanes = slice(half * 128, half * 128 + 128)
        both = jnp.where(row == xs, log_sum[:, lanes], both)
        both = jnp.where(row == xs + NX, picked[:, lanes], both)
    out_ref[...] = jnp.broadcast_to(both[None], out_ref.shape) if last else both


def close_kernel(pieces_ref, loss_ref, sum_ref):
    log_sum = pieces_ref[:, :NX, :]
    peak = jnp.max(log_sum, axis=0)
    total = jnp.sum(jnp.exp(log_sum - peak[None]), axis=0)
    loss = peak + jnp.log(total) - jnp.sum(pieces_ref[:, NX:, :], axis=0)
    loss_ref[...] = loss
    summed = jnp.sum(jnp.sum(loss, axis=0, keepdims=True), axis=1, keepdims=True)
    sum_ref[...] = jnp.broadcast_to(summed[None], sum_ref.shape)


def on_device(hidden, embedding, logit_scale, targets):
    rows = embedding.shape[0]
    index = lax.axis_index("vocab")
    x, z, core = place(index)
    swapped = shift(embedding, 0, 0, 1)
    any_space = pl.BlockSpec(memory_space=pltpu.HBM)
    unit, a, b = call(
        unit_kernel,
        (
            pltpu.VMEM((ROWS, D + CT), bf16),
            pltpu.VMEM((ROWS, CA), bf16),
            pltpu.VMEM((ROWS, CB + CT), bf16),
        ),
        "unit",
        58 << 20,
        (
            pltpu.VMEM((ROWS, D), bf16),
            pltpu.VMEM((1, ROWS), jnp.int32),
            pltpu.SemaphoreType.DMA((2,)),
        ),
        specs=[any_space, any_space],
    )(hidden, targets.reshape(1, ROWS))
    swapped_scale = shift(logit_scale.reshape(rows // 128, 128), 0, 0, 1)

    a_far = shift(a, 2, 0)
    left, right = shift(unit, 1, 0), shift(unit, -1, 0)
    b1, c1, b2, c2 = shift(b, 0, 1), shift(b, 0, -1), shift(b, 0, 2), shift(b, 0, -2)
    line = jnp.concatenate([left[:, :CA], right[:, :CA], a, a_far], axis=1)
    near = jnp.concatenate([b1, c1, b2, c2])
    q1, n1 = shift(near, 1, 0), shift(near, -1, 0)
    wide = NX * CA
    line_b, line_c = jnp.concatenate([line, b2], axis=1), jnp.concatenate([line, c2], axis=1)
    p1, m1 = shift(line_b, 0, 1), shift(line_c, 0, -1)
    p2, m2 = shift(line_b, 0, 2), shift(line, 0, -2)
    b3, c3, b4 = p1[:, wide:], m1[:, wide:], p2[:, wide:]
    apart = jnp.concatenate([b3, c3, b4])
    q2, n2 = shift(apart, 1, 0), shift(apart, -1, 0)
    p2_line = p2[:, :wide]
    p3, m3, p4 = shift(p2_line, 0, 1), shift(m2, 0, -1), shift(p2_line, 0, 2)
    q3 = shift(q1, 1, 0)
    n3 = shift(jnp.concatenate([right[:, CA:], n2]), -1, 0)

    lines = (line, p1, m1, p2, m2, p3, m3, p4)
    line_dz = (0, -1, 1, -2, 2, -3, 3, -4)
    near_dz, apart_dz = (-1, 1, -2, 2), (-3, 3, -4)

    def spots(buffer, half, offsets, column=0):
        return [(buffer, k * ROWS, column, half, dz) for k, dz in enumerate(offsets)]

    cost = pl.CostEstimate(
        flops=2 * 2 * rows * D * 256, bytes_accessed=16 * rows * D, transcendentals=0
    )
    scratch = (
        pltpu.VMEM((256, D), bf16),
        pltpu.VMEM((256, CT), f32),
        pltpu.VMEM((2 * rows, 256), f32),
    )

    def head(a_spots, b_spots, given, specs, sources, name):
        last = name == "head_column"
        piece = jax.ShapeDtypeStruct((NX * NZ, 8, 128) if last else (8, 128), f32)
        kept = (pltpu.VMEM((2 * rows, D), bf16), pltpu.VMEM((2 * rows, 128), f32))
        more = (
            pltpu.VMEM((2 * rows // 128, 128), f32),
            pltpu.SemaphoreType.DMA((2 * rows // BLOCK + 1,)),
        )
        return call(
            functools.partial(head_kernel, a_spots, b_spots, last, (len(lines), len(sources))),
            piece if last else (piece, *kept),
            name,
            28 << 20,
            scratch if last else scratch + more,
            cost,
            specs + [VMEM] * (len(lines) + len(sources)),
        )(*given, *lines, *sources)

    a_spots = [(k, 0, half * CA, half, dz) for k, dz in enumerate(line_dz) for half in (0, 1)]
    b_spots = []
    for half in (0, 1):
        b_spots += spots(3 * half, half, (0,), CA)
        b_spots += spots(3 * half + 1, half, near_dz)
        b_spots += spots(3 * half + 2, half, apart_dz)
    sides = (left, q1, q2, right, n1, n2)
    given = (embedding, swapped, logit_scale.reshape(rows // 128, 128), swapped_scale)
    specs = [any_space] * 3 + [VMEM]
    first, tables, gains = head(a_spots, b_spots, given, specs, sides, "head_sides")
    a_spots = [
        (k, 0, (2 + half) * CA, half, dz) for k, dz in enumerate(line_dz) for half in (0, 1)
    ]
    b_spots = spots(0, 0, (0,)) + spots(1, 0, near_dz) + spots(2, 0, apart_dz)
    b_spots += spots(3, 1, near_dz) + spots(4, 1, (0,) + apart_dz)
    columns = (b, near, apart, q3, n3)
    given = (tables, gains, first)
    pieces = head(a_spots, b_spots, given, [VMEM] * 3, columns, "head_column")

    same_core = [[v for v in range(NX * NZ * NC) if v % NC == c] for c in range(NC)]
    pieces = lax.all_to_all(pieces, "vocab", 0, 0, tiled=True, axis_index_groups=same_core)
    loss, summed = call(
        close_kernel,
        (jax.ShapeDtypeStruct((NX, 128), f32), jax.ShapeDtypeStruct((NY * NC, 1, 128), f32)),
        "close",
        4 << 20,
    )(pieces)
    groups = [
        [(v + c) * NY + s for c in range(NC) for s in range(NY)]
        for v in range(0, NX * NZ * NC, NC)
    ]
    summed = lax.all_to_all(summed, ("vocab", "seq"), 0, 0, tiled=True, axis_index_groups=groups)
    mean_loss = jnp.sum(summed[:, 0, 0]) / (NX * NZ * NC * NY * ROWS)
    own_loss = lax.dynamic_slice(loss, (x, z * ROWS), (1, ROWS)).reshape(ROWS)
    return own_loss, mean_loss


def solution(mesh):
    in_specs = (P(("vocab", "seq"), None), P("vocab", None), P("vocab"), P(("vocab", "seq")))
    out_specs = (P(("vocab", "seq")), P())
    return jax.shard_map(
        on_device, mesh=mesh, in_specs=in_specs, out_specs=out_specs, check_vma=False
    )
```

```python
import functools

import jax
import jax.numpy as jnp
from jax import lax
from jax.experimental import pallas as pl
from jax.experimental.pallas import tpu as pltpu
from jax.sharding import PartitionSpec as P

epsilon = 1e-06
NX, NZ, NC, NY = 4, 8, 2, 4
D = 4096
CA = 1024
CB = D - CA
CT = 128
ROWS = 16
HALF = NZ * ROWS
BLOCK = 512
f32, bf16 = jnp.float32, jnp.bfloat16
VMEM = pl.BlockSpec(memory_space=pltpu.VMEM)


def index_of(x, z, core):
    return ((x % NX) * NZ + z % NZ) * NC + core


def shift(array, dx, dz, flip=0):
    pairs = [
        (index_of(x, z, c), index_of(x + dx, z + dz, c ^ flip))
        for x in range(NX)
        for z in range(NZ)
        for c in range(NC)
    ]
    return lax.ppermute(array, "vocab", pairs)


def call(kernel, out_shape, name, limit, scratch=(), cost=None, specs=None):
    return lambda *args: pl.pallas_call(
        kernel,
        out_shape=out_shape,
        in_specs=specs or [VMEM] * len(args),
        out_specs=jax.tree.map(lambda _: VMEM, out_shape),
        scratch_shapes=list(scratch),
        compiler_params=pltpu.CompilerParams(vmem_limit_bytes=limit),
        cost_estimate=cost,
        name=name,
    )(*args)


def unit_kernel(
    hidden_hbm, target_hbm, scale_hbm, unit_ref, a_ref, b_ref, scale_ref, hidden_ref, target_ref, arrived
):
    copies = (
        pltpu.make_async_copy(scale_hbm, scale_ref, arrived.at[2]),
        pltpu.make_async_copy(hidden_hbm, hidden_ref, arrived.at[0]),
        pltpu.make_async_copy(target_hbm, target_ref, arrived.at[1]),
    )
    for copy in copies:
        copy.start()
    for copy in copies:
        copy.wait()
    wide = hidden_ref[...].astype(f32)
    unit = wide * lax.rsqrt(jnp.sum(wide * wide, axis=1, keepdims=True) + epsilon)
    unit = unit.astype(bf16)
    row = lax.broadcasted_iota(jnp.int32, (ROWS, ROWS), 0)
    column = lax.broadcasted_iota(jnp.int32, (ROWS, ROWS), 1)
    target = jnp.where(row == column, jnp.broadcast_to(target_ref[...], (ROWS, ROWS)), 0)
    high = jnp.sum((target // 256).astype(f32), axis=1, keepdims=True)
    low = jnp.sum((target % 256).astype(f32), axis=1, keepdims=True)
    lane = lax.broadcasted_iota(jnp.int32, (ROWS, CT), 1)
    coded = jnp.where(lane == 0, high, jnp.where(lane == 1, low, 0.0)).astype(bf16)
    unit_ref[:, :D] = unit
    unit_ref[:, D:] = coded
    a_ref[...] = unit[:, :CA]
    b_ref[:, :CB] = unit[:, CA:]
    b_ref[:, CB:] = coded


def place(index):
    core = index % NC
    z = (index // NC) % NZ
    return index // (NC * NZ), z, core


def head_kernel(a_spots, b_spots, last, counts, *refs):
    n_a, n_b = counts
    if last:
        tables, gains, first_ref, *rest = refs
    else:
        own_ref, swapped_ref, own_scale, swapped_scale, *rest = refs
    a_refs, b_refs, rest = rest[:n_a], rest[n_a : n_a + n_b], rest[n_a + n_b :]
    if last:
        out_ref, tokens, coded, logits = rest
    else:
        out_ref, tables, gains, tokens, coded, logits, scales, arrived = rest
    rows = tables.shape[0] // 2
    blocks = 2 * rows // BLOCK

    if not last:
        for k in range(blocks):
            source = (own_ref, swapped_ref)[k * BLOCK // rows]
            at = pl.ds(k * BLOCK % rows, BLOCK)
            pltpu.make_async_copy(
                source.at[at], tables.at[pl.ds(k * BLOCK, BLOCK)], arrived.at[k]
            ).start()
        scales[: rows // 128, :] = own_scale[...]
        scales[rows // 128 :, :] = swapped_scale[...]
    index = lax.axis_index("vocab")
    x, z, core = place(index)

    def spot(half, dz):
        return pl.ds(pl.multiple_of(half * HALF + lax.rem(z + dz + NZ, NZ) * ROWS, ROWS), ROWS)

    for buffer, row, column, half, dz in a_spots:
        tokens[spot(half, dz), :CA] = a_refs[buffer][row : row + ROWS, column : column + CA]
    for buffer, row, column, half, dz in b_spots:
        ref = b_refs[buffer]
        tokens[spot(half, dz), CA:] = ref[row : row + ROWS, column : column + CB]
        coded[spot(half, dz), :] = ref[row : row + ROWS, column + CB : column + CB + CT].astype(f32)
    code = coded[...].T
    target = (code[0:1, :] * 256.0 + code[1:2, :]).astype(jnp.int32)
    own_base, swapped_base = index * rows, (index - 2 * core) * rows

    def step(k, carry):
        peak, picked = carry
        part = pl.ds(pl.multiple_of(k * BLOCK, BLOCK), BLOCK)
        if not last:
            pltpu.make_async_copy(own_ref.at[pl.ds(0, BLOCK)], tables.at[part], arrived.at[k]).wait()
            for j in range(BLOCK // 128):
                some = pl.ds(pl.multiple_of(k * BLOCK + j * 128, 128), 128)
                total = jnp.zeros((128, 128), f32)
                for i in range(D // 128):
                    piece = tables[some, i * 128 : (i + 1) * 128].astype(f32)
                    total += piece * piece
                norm = lax.rsqrt(jnp.sum(total, axis=1, keepdims=True) + epsilon)
                scale = scales[pl.ds(k * (BLOCK // 128) + j, 1), :]
                gains[some, :] = norm * jnp.broadcast_to(scale, (128, 128)).T
        value = lax.dot_general(
            tables[part, :], tokens[...], (((1,), (1,)), ((), ())), preferred_element_type=f32
        )
        factor = gains[part, :]
        value = value * jnp.concatenate([factor, factor], axis=1)
        logits[part, :] = value
        base = jnp.where(k * BLOCK < rows, own_base, swapped_base) + k * BLOCK
        row = lax.broadcasted_iota(jnp.int32, (BLOCK, 256), 0)
        chosen = jnp.where(row == target - base, value, 0.0)
        peak = jnp.maximum(peak, jnp.max(value.reshape(BLOCK // 8, 8, 256), axis=0))
        picked = picked + jnp.sum(chosen.reshape(BLOCK // 8, 8, 256), axis=0)
        return peak, picked

    peak, picked = lax.fori_loop(
        0, blocks, step, (jnp.full((8, 256), -jnp.inf, f32), jnp.zeros((8, 256), f32))
    )
    peak = jnp.max(peak, axis=0, keepdims=True)

    def add(k, total):
        part = pl.ds(pl.multiple_of(k * 256, 256), 256)
        term = jnp.exp(logits[part, :] - peak)
        return total + jnp.sum(term.reshape(32, 8, 256), axis=0)

    total = lax.fori_loop(0, 2 * rows // 256, add, jnp.zeros((8, 256), f32))
    log_sum = peak + jnp.log(jnp.sum(total, axis=0, keepdims=True))
    picked = jnp.sum(picked, axis=0, keepdims=True)
    row = lax.broadcasted_iota(jnp.int32, (8, 128), 0)
    both = first_ref[...] if last else jnp.zeros((8, 128), f32)
    for half, dx in enumerate((0, 2) if last else (-1, 1)):
        xs = lax.rem(x + dx + NX, NX)
        lanes = slice(half * 128, half * 128 + 128)
        both = jnp.where(row == xs, log_sum[:, lanes], both)
        both = jnp.where(row == xs + NX, picked[:, lanes], both)
    out_ref[...] = jnp.broadcast_to(both[None], out_ref.shape) if last else both


def close_kernel(pieces_ref, loss_ref, sum_ref):
    log_sum = pieces_ref[:, :NX, :]
    peak = jnp.max(log_sum, axis=0)
    total = jnp.sum(jnp.exp(log_sum - peak[None]), axis=0)
    loss = peak + jnp.log(total) - jnp.sum(pieces_ref[:, NX:, :], axis=0)
    loss_ref[...] = loss
    summed = jnp.sum(jnp.sum(loss, axis=0, keepdims=True), axis=1, keepdims=True)
    sum_ref[...] = jnp.broadcast_to(summed[None], sum_ref.shape)


def on_device(hidden, embedding, logit_scale, targets):
    rows = embedding.shape[0]
    index = lax.axis_index("vocab")
    x, z, core = place(index)
    swapped = shift(embedding, 0, 0, 1)
    any_space = pl.BlockSpec(memory_space=pltpu.HBM)
    unit, a, b, own_scale = call(
        unit_kernel,
        (
            pltpu.VMEM((ROWS, D + CT), bf16),
            pltpu.VMEM((ROWS, CA), bf16),
            pltpu.VMEM((ROWS, CB + CT), bf16),
            pltpu.VMEM((rows // 128, 128), f32),
        ),
        "unit",
        58 << 20,
        (
            pltpu.VMEM((ROWS, D), bf16),
            pltpu.VMEM((1, ROWS), jnp.int32),
            pltpu.SemaphoreType.DMA((3,)),
        ),
        specs=[any_space] * 3,
    )(hidden, targets.reshape(1, ROWS), logit_scale.reshape(rows // 128, 128))
    swapped_scale = shift(own_scale, 0, 0, 1)

    a_far = shift(a, 2, 0)
    left, right = shift(unit, 1, 0), shift(unit, -1, 0)
    b1, c1, b2, c2 = shift(b, 0, 1), shift(b, 0, -1), shift(b, 0, 2), shift(b, 0, -2)
    line = jnp.concatenate([left[:, :CA], right[:, :CA], a, a_far])
    p1, m1 = shift(line, 0, 1), shift(line, 0, -1)
    near = jnp.concatenate([b1, c1, b2, c2])
    q1, n1 = shift(near, 1, 0), shift(near, -1, 0)
    p2, m2 = shift(line, 0, 2), shift(line, 0, -2)
    b3, c3, b4 = shift(b2, 0, 1), shift(c2, 0, -1), shift(b2, 0, 2)
    p3, m3, p4 = shift(p2, 0, 1), shift(m2, 0, -1), shift(p2, 0, 2)
    apart = jnp.concatenate([b3, c3, b4])
    q2, n2 = shift(apart, 1, 0), shift(apart, -1, 0)
    q3 = shift(q1, 1, 0)
    n3 = shift(jnp.concatenate([right[:, CA:], n2]), -1, 0)

    lines = (line, p1, m1, p2, m2, p3, m3, p4)
    line_dz = (0, -1, 1, -2, 2, -3, 3, -4)
    near_dz, apart_dz = (-1, 1, -2, 2), (-3, 3, -4)

    def spots(buffer, half, offsets, column=0):
        return [(buffer, k * ROWS, column, half, dz) for k, dz in enumerate(offsets)]

    cost = pl.CostEstimate(
        flops=2 * 2 * rows * D * 256, bytes_accessed=16 * rows * D, transcendentals=0
    )
    scratch = (
        pltpu.VMEM((256, D), bf16),
        pltpu.VMEM((256, CT), f32),
        pltpu.VMEM((2 * rows, 256), f32),
    )

    def head(a_spots, b_spots, given, specs, sources, name):
        last = name == "head_column"
        piece = jax.ShapeDtypeStruct((NX * NZ, 8, 128) if last else (8, 128), f32)
        kept = (pltpu.VMEM((2 * rows, D), bf16), pltpu.VMEM((2 * rows, 128), f32))
        more = (
            pltpu.VMEM((2 * rows // 128, 128), f32),
            pltpu.SemaphoreType.DMA((2 * rows // BLOCK,)),
        )
        return call(
            functools.partial(head_kernel, a_spots, b_spots, last, (len(lines), len(sources))),
            piece if last else (piece, *kept),
            name,
            28 << 20,
            scratch if last else scratch + more,
            cost,
            specs + [VMEM] * (len(lines) + len(sources)),
        )(*given, *lines, *sources)

    a_spots = [(k, half * ROWS, 0, half, dz) for k, dz in enumerate(line_dz) for half in (0, 1)]
    b_spots = []
    for half in (0, 1):
        b_spots += spots(3 * half, half, (0,), CA)
        b_spots += spots(3 * half + 1, half, near_dz)
        b_spots += spots(3 * half + 2, half, apart_dz)
    sides = (left, q1, q2, right, n1, n2)
    given = (embedding, swapped, own_scale, swapped_scale)
    specs = [any_space] * 2 + [VMEM] * 2
    first, tables, gains = head(a_spots, b_spots, given, specs, sides, "head_sides")
    a_spots = [
        (k, (2 + half) * ROWS, 0, half, dz) for k, dz in enumerate(line_dz) for half in (0, 1)
    ]
    b_spots = spots(0, 0, (0,)) + spots(1, 0, near_dz) + spots(2, 0, apart_dz)
    b_spots += spots(3, 1, near_dz) + spots(4, 1, (0,) + apart_dz)
    columns = (b, near, apart, q3, n3)
    given = (tables, gains, first)
    pieces = head(a_spots, b_spots, given, [VMEM] * 3, columns, "head_column")

    same_core = [[v for v in range(NX * NZ * NC) if v % NC == c] for c in range(NC)]
    pieces = lax.all_to_all(pieces, "vocab", 0, 0, tiled=True, axis_index_groups=same_core)
    loss, summed = call(
        close_kernel,
        (jax.ShapeDtypeStruct((NX, 128), f32), jax.ShapeDtypeStruct((NY * NC, 1, 128), f32)),
        "close",
        4 << 20,
    )(pieces)
    groups = [
        [(v + c) * NY + s for c in range(NC) for s in range(NY)]
        for v in range(0, NX * NZ * NC, NC)
    ]
    summed = lax.all_to_all(summed, ("vocab", "seq"), 0, 0, tiled=True, axis_index_groups=groups)
    mean_loss = jnp.sum(summed[:, 0, 0]) / (NX * NZ * NC * NY * ROWS)
    own_loss = lax.dynamic_slice(loss, (x, z * ROWS), (1, ROWS)).reshape(ROWS)
    return own_loss, mean_loss


def solution(mesh):
    in_specs = (P(("vocab", "seq"), None), P("vocab", None), P("vocab"), P(("vocab", "seq")))
    out_specs = (P(("vocab", "seq")), P())
    return jax.shard_map(
        on_device, mesh=mesh, in_specs=in_specs, out_specs=out_specs, check_vma=False
    )
```

```python
import functools

import jax
import jax.numpy as jnp
from jax import lax
from jax.experimental import pallas as pl
from jax.experimental.pallas import tpu as pltpu
from jax.sharding import PartitionSpec as P


epsilon = 1e-06
NX, NZ, NC, NY = 4, 8, 2, 4
D = 4096
CA = 1024
CB = D - CA
CT = 128
ROWS = 16
HALF = NZ * ROWS
BLOCK = 512
f32, bf16 = jnp.float32, jnp.bfloat16
VMEM = pl.BlockSpec(memory_space=pltpu.VMEM)


def index_of(x, z, core):
    return ((x % NX) * NZ + z % NZ) * NC + core


def shift(array, dx, dz, flip=0):
    pairs = [
        (index_of(x, z, c), index_of(x + dx, z + dz, c ^ flip))
        for x in range(NX)
        for z in range(NZ)
        for c in range(NC)
    ]
    return lax.ppermute(array, "vocab", pairs)


def call(kernel, out_shape, limit, scratch=(), cost=None, specs=None):
    return lambda *args: pl.pallas_call(
        kernel,
        out_shape=out_shape,
        in_specs=specs or [VMEM] * len(args),
        out_specs=jax.tree.map(lambda _: VMEM, out_shape),
        scratch_shapes=list(scratch),
        compiler_params=pltpu.CompilerParams(vmem_limit_bytes=limit),
        cost_estimate=cost,
    )(*args)


def unit_kernel(
    hidden_hbm, target_hbm, scale_hbm, unit_ref, a_ref, b_ref, scale_ref, hidden_ref, target_ref, arrived
):
    copies = (
        pltpu.make_async_copy(scale_hbm, scale_ref, arrived.at[2]),
        pltpu.make_async_copy(hidden_hbm, hidden_ref, arrived.at[0]),
        pltpu.make_async_copy(target_hbm, target_ref, arrived.at[1]),
    )
    for copy in copies:
        copy.start()
    for copy in copies:
        copy.wait()
    wide = hidden_ref[...].astype(f32)
    unit = wide * lax.rsqrt(jnp.sum(wide * wide, axis=1, keepdims=True) + epsilon)
    unit = unit.astype(bf16)
    row = lax.broadcasted_iota(jnp.int32, (ROWS, ROWS), 0)
    column = lax.broadcasted_iota(jnp.int32, (ROWS, ROWS), 1)
    target = jnp.where(row == column, jnp.broadcast_to(target_ref[...], (ROWS, ROWS)), 0)
    high = jnp.sum((target // 256).astype(f32), axis=1, keepdims=True)
    low = jnp.sum((target % 256).astype(f32), axis=1, keepdims=True)
    lane = lax.broadcasted_iota(jnp.int32, (ROWS, CT), 1)
    coded = jnp.where(lane == 0, high, jnp.where(lane == 1, low, 0.0)).astype(bf16)
    unit_ref[:, :D] = unit
    unit_ref[:, D:] = coded
    a_ref[...] = unit[:, :CA]
    b_ref[:, :CB] = unit[:, CA:]
    b_ref[:, CB:] = coded


def place(index):
    core = index % NC
    z = (index // NC) % NZ
    return index // (NC * NZ), z, core


def head_kernel(a_spots, b_spots, last, counts, *refs):
    n_a, n_b = counts
    if last:
        tables, gains, first_ref, *rest = refs
    else:
        own_ref, swapped_ref, own_scale, swapped_scale, *rest = refs
    a_refs, b_refs, rest = rest[:n_a], rest[n_a : n_a + n_b], rest[n_a + n_b :]
    if last:
        out_ref, tokens, coded, logits = rest
    else:
        out_ref, tables, gains, tokens, coded, logits, scales, arrived = rest
    rows = tables.shape[0] // 2
    blocks = 2 * rows // BLOCK

    if not last:
        for k in range(blocks):
            source = (own_ref, swapped_ref)[k * BLOCK // rows]
            at = pl.ds(k * BLOCK % rows, BLOCK)
            pltpu.make_async_copy(
                source.at[at], tables.at[pl.ds(k * BLOCK, BLOCK)], arrived.at[k]
            ).start()
        scales[: rows // 128, :] = own_scale[...]
        scales[rows // 128 :, :] = swapped_scale[...]
    index = lax.axis_index("vocab")
    x, z, core = place(index)

    def spot(half, dz):
        return pl.ds(pl.multiple_of(half * HALF + lax.rem(z + dz + NZ, NZ) * ROWS, ROWS), ROWS)

    for buffer, row, column, half, dz in a_spots:
        tokens[spot(half, dz), :CA] = a_refs[buffer][row : row + ROWS, column : column + CA]
    for buffer, row, column, half, dz in b_spots:
        ref = b_refs[buffer]
        tokens[spot(half, dz), CA:] = ref[row : row + ROWS, column : column + CB]
        coded[spot(half, dz), :] = ref[row : row + ROWS, column + CB : column + CB + CT].astype(f32)
    code = coded[...].T
    target = (code[0:1, :] * 256.0 + code[1:2, :]).astype(jnp.int32)
    own_base, swapped_base = index * rows, (index - 2 * core) * rows

    def step(k, carry):
        peak, picked = carry
        part = pl.ds(pl.multiple_of(k * BLOCK, BLOCK), BLOCK)
        if not last:
            pltpu.make_async_copy(own_ref.at[pl.ds(0, BLOCK)], tables.at[part], arrived.at[k]).wait()
            for j in range(BLOCK // 128):
                some = pl.ds(pl.multiple_of(k * BLOCK + j * 128, 128), 128)
                total = jnp.zeros((128, 128), f32)
                for i in range(D // 128):
                    piece = tables[some, i * 128 : (i + 1) * 128].astype(f32)
                    total += piece * piece
                norm = lax.rsqrt(jnp.sum(total, axis=1, keepdims=True) + epsilon)
                scale = scales[pl.ds(k * (BLOCK // 128) + j, 1), :]
                gains[some, :] = norm * jnp.broadcast_to(scale, (128, 128)).T
        value = lax.dot_general(
            tables[part, :], tokens[...], (((1,), (1,)), ((), ())), preferred_element_type=f32
        )
        factor = gains[part, :]
        value = value * jnp.concatenate([factor, factor], axis=1)
        logits[part, :] = value
        base = jnp.where(k * BLOCK < rows, own_base, swapped_base) + k * BLOCK
        row = lax.broadcasted_iota(jnp.int32, (BLOCK, 256), 0)
        chosen = jnp.where(row == target - base, value, 0.0)
        peak = jnp.maximum(peak, jnp.max(value.reshape(BLOCK // 8, 8, 256), axis=0))
        picked = picked + jnp.sum(chosen.reshape(BLOCK // 8, 8, 256), axis=0)
        return peak, picked

    peak, picked = lax.fori_loop(
        0, blocks, step, (jnp.full((8, 256), -jnp.inf, f32), jnp.zeros((8, 256), f32))
    )
    peak = jnp.max(peak, axis=0, keepdims=True)

    def add(k, total):
        part = pl.ds(pl.multiple_of(k * 256, 256), 256)
        term = jnp.exp(logits[part, :] - peak)
        return total + jnp.sum(term.reshape(32, 8, 256), axis=0)

    total = lax.fori_loop(0, 2 * rows // 256, add, jnp.zeros((8, 256), f32))
    log_sum = peak + jnp.log(jnp.sum(total, axis=0, keepdims=True))
    picked = jnp.sum(picked, axis=0, keepdims=True)
    row = lax.broadcasted_iota(jnp.int32, (8, 128), 0)
    both = first_ref[...] if last else jnp.zeros((8, 128), f32)
    for half, dx in enumerate((0, 2) if last else (-1, 1)):
        xs = lax.rem(x + dx + NX, NX)
        lanes = slice(half * 128, half * 128 + 128)
        both = jnp.where(row == xs, log_sum[:, lanes], both)
        both = jnp.where(row == xs + NX, picked[:, lanes], both)
    out_ref[...] = jnp.broadcast_to(both[None], out_ref.shape) if last else both


def close_kernel(pieces_ref, loss_ref, sum_ref):
    log_sum = pieces_ref[:, :NX, :]
    peak = jnp.max(log_sum, axis=0)
    total = jnp.sum(jnp.exp(log_sum - peak[None]), axis=0)
    loss = peak + jnp.log(total) - jnp.sum(pieces_ref[:, NX:, :], axis=0)
    loss_ref[...] = loss
    summed = jnp.sum(jnp.sum(loss, axis=0, keepdims=True), axis=1, keepdims=True)
    sum_ref[...] = jnp.broadcast_to(summed[None], sum_ref.shape)


def head_loss(hidden, embedding, logit_scale, targets):
    rows = embedding.shape[0]
    index = lax.axis_index("vocab")
    x, z, _ = place(index)
    swapped = shift(embedding, 0, 0, 1)
    any_space = pl.BlockSpec(memory_space=pltpu.HBM)
    unit, a, b, own_scale = call(
        unit_kernel,
        (
            pltpu.VMEM((ROWS, D + CT), bf16),
            pltpu.VMEM((ROWS, CA), bf16),
            pltpu.VMEM((ROWS, CB + CT), bf16),
            pltpu.VMEM((rows // 128, 128), f32),
        ),
        58 << 20,
        (
            pltpu.VMEM((ROWS, D), bf16),
            pltpu.VMEM((1, ROWS), jnp.int32),
            pltpu.SemaphoreType.DMA((3,)),
        ),
        specs=[any_space] * 3,
    )(hidden, targets.reshape(1, ROWS), logit_scale.reshape(rows // 128, 128))
    swapped_scale = shift(own_scale, 0, 0, 1)

    a_far = shift(a, 2, 0)
    left, right = shift(unit, 1, 0), shift(unit, -1, 0)
    b1, c1, b2, c2 = shift(b, 0, 1), shift(b, 0, -1), shift(b, 0, 2), shift(b, 0, -2)
    line = jnp.concatenate([left[:, :CA], right[:, :CA], a, a_far])
    p1, m1 = shift(line, 0, 1), shift(line, 0, -1)
    near = jnp.concatenate([b1, c1, b2, c2])
    q1, n1 = shift(near, 1, 0), shift(near, -1, 0)
    p2, m2 = shift(line, 0, 2), shift(line, 0, -2)
    b3, c3, b4 = shift(b2, 0, 1), shift(c2, 0, -1), shift(b2, 0, 2)
    p3, m3, p4 = shift(p2, 0, 1), shift(m2, 0, -1), shift(p2, 0, 2)
    apart = jnp.concatenate([b3, c3, b4])
    q2, n2 = shift(apart, 1, 0), shift(apart, -1, 0)
    q3 = shift(q1, 1, 0)
    n3 = shift(jnp.concatenate([right[:, CA:], n2]), -1, 0)

    lines = (line, p1, m1, p2, m2, p3, m3, p4)
    line_dz = (0, -1, 1, -2, 2, -3, 3, -4)
    near_dz, apart_dz = (-1, 1, -2, 2), (-3, 3, -4)

    def spots(buffer, half, offsets, column=0):
        return [(buffer, k * ROWS, column, half, dz) for k, dz in enumerate(offsets)]

    cost = pl.CostEstimate(
        flops=2 * 2 * rows * D * 256, bytes_accessed=16 * rows * D, transcendentals=0
    )
    scratch = (
        pltpu.VMEM((256, D), bf16),
        pltpu.VMEM((256, CT), f32),
        pltpu.VMEM((2 * rows, 256), f32),
    )

    def head(a_spots, b_spots, given, specs, sources, name):
        last = name == "head_column"
        piece = jax.ShapeDtypeStruct((NX * NZ, 8, 128) if last else (8, 128), f32)
        kept = (pltpu.VMEM((2 * rows, D), bf16), pltpu.VMEM((2 * rows, 128), f32))
        more = (
            pltpu.VMEM((2 * rows // 128, 128), f32),
            pltpu.SemaphoreType.DMA((2 * rows // BLOCK,)),
        )
        return call(
            functools.partial(head_kernel, a_spots, b_spots, last, (len(lines), len(sources))),
            piece if last else (piece, *kept),
            28 << 20,
            scratch if last else scratch + more,
            cost,
            specs + [VMEM] * (len(lines) + len(sources)),
        )(*given, *lines, *sources)

    a_spots = [(k, half * ROWS, 0, half, dz) for k, dz in enumerate(line_dz) for half in (0, 1)]
    b_spots = []
    for half in (0, 1):
        b_spots += spots(3 * half, half, (0,), CA)
        b_spots += spots(3 * half + 1, half, near_dz)
        b_spots += spots(3 * half + 2, half, apart_dz)
    sides = (left, q1, q2, right, n1, n2)
    given = (embedding, swapped, own_scale, swapped_scale)
    specs = [any_space] * 2 + [VMEM] * 2
    first, tables, gains = head(a_spots, b_spots, given, specs, sides, "head_sides")
    a_spots = [
        (k, (2 + half) * ROWS, 0, half, dz) for k, dz in enumerate(line_dz) for half in (0, 1)
    ]
    b_spots = spots(0, 0, (0,)) + spots(1, 0, near_dz) + spots(2, 0, apart_dz)
    b_spots += spots(3, 1, near_dz) + spots(4, 1, (0,) + apart_dz)
    columns = (b, near, apart, q3, n3)
    given = (tables, gains, first)
    pieces = head(a_spots, b_spots, given, [VMEM] * 3, columns, "head_column")

    same_core = [[v for v in range(NX * NZ * NC) if v % NC == c] for c in range(NC)]
    pieces = lax.all_to_all(pieces, "vocab", 0, 0, tiled=True, axis_index_groups=same_core)
    loss, summed = call(
        close_kernel,
        (jax.ShapeDtypeStruct((NX, 128), f32), jax.ShapeDtypeStruct((NY * NC, 1, 128), f32)),
        4 << 20,
    )(pieces)
    groups = [
        [(v + c) * NY + s for c in range(NC) for s in range(NY)]
        for v in range(0, NX * NZ * NC, NC)
    ]
    summed = lax.all_to_all(summed, ("vocab", "seq"), 0, 0, tiled=True, axis_index_groups=groups)
    mean_loss = jnp.sum(summed[:, 0, 0]) / (NX * NZ * NC * NY * ROWS)
    own_loss = lax.dynamic_slice(loss, (x, z * ROWS), (1, ROWS)).reshape(ROWS)
    return own_loss, mean_loss


def solution(mesh):
    in_specs = (P(("vocab", "seq"), None), P("vocab", None), P("vocab"), P(("vocab", "seq")))
    out_specs = (P(("vocab", "seq")), P())
    return jax.shard_map(
        head_loss, mesh=mesh, in_specs=in_specs, out_specs=out_specs, check_vma=False
    )
```

```python
import functools

import jax
import jax.numpy as jnp
from jax import lax
from jax.experimental import pallas as pl
from jax.experimental.pallas import tpu as pltpu
from jax.sharding import PartitionSpec as P


epsilon = 1e-06
NX, NZ, NC, NY = 4, 8, 2, 4
D = 4096
CA = 768
CB = D - CA
CT = 128
ROWS = 16
HALF = NZ * ROWS
BLOCK = 256
f32, bf16 = jnp.float32, jnp.bfloat16
VMEM = pl.BlockSpec(memory_space=pltpu.VMEM)


def index_of(x, z, core):
    return ((x % NX) * NZ + z % NZ) * NC + core


def shift(array, dx, dz, flip=0):
    pairs = [
        (index_of(x, z, c), index_of(x + dx, z + dz, c ^ flip))
        for x in range(NX)
        for z in range(NZ)
        for c in range(NC)
    ]
    return lax.ppermute(array, "vocab", pairs)


def call(kernel, out_shape, limit, scratch=(), cost=None, specs=None):
    return lambda *args: pl.pallas_call(
        kernel,
        out_shape=out_shape,
        in_specs=specs or [VMEM] * len(args),
        out_specs=jax.tree.map(lambda _: VMEM, out_shape),
        scratch_shapes=list(scratch),
        compiler_params=pltpu.CompilerParams(vmem_limit_bytes=limit),
        cost_estimate=cost,
    )(*args)


def unit_kernel(
    hidden_hbm, target_hbm, scale_hbm, unit_ref, a_ref, b_ref, scale_ref, hidden_ref, target_ref, arrived
):
    copies = (
        pltpu.make_async_copy(scale_hbm, scale_ref, arrived.at[2]),
        pltpu.make_async_copy(hidden_hbm, hidden_ref, arrived.at[0]),
        pltpu.make_async_copy(target_hbm, target_ref, arrived.at[1]),
    )
    for copy in copies:
        copy.start()
    for copy in copies:
        copy.wait()
    wide = hidden_ref[...].astype(f32)
    unit = wide * lax.rsqrt(jnp.sum(wide * wide, axis=1, keepdims=True) + epsilon)
    unit = unit.astype(bf16)
    row = lax.broadcasted_iota(jnp.int32, (ROWS, ROWS), 0)
    column = lax.broadcasted_iota(jnp.int32, (ROWS, ROWS), 1)
    target = jnp.where(row == column, jnp.broadcast_to(target_ref[...], (ROWS, ROWS)), 0)
    high = jnp.sum((target // 256).astype(f32), axis=1, keepdims=True)
    low = jnp.sum((target % 256).astype(f32), axis=1, keepdims=True)
    lane = lax.broadcasted_iota(jnp.int32, (ROWS, CT), 1)
    coded = jnp.where(lane == 0, high, jnp.where(lane == 1, low, 0.0)).astype(bf16)
    unit_ref[:, :D] = unit
    unit_ref[:, D:] = coded
    a_ref[...] = unit[:, :CA]
    b_ref[:, :CB] = unit[:, CA:]
    b_ref[:, CB:] = coded


def place(index):
    core = index % NC
    z = (index // NC) % NZ
    return index // (NC * NZ), z, core


def head_kernel(a_spots, b_spots, last, counts, *refs):
    n_a, n_b = counts
    block = 4 * BLOCK if last else BLOCK
    if last:
        tables, gains, first_ref, *rest = refs
    else:
        own_ref, swapped_ref, own_scale, swapped_scale, *rest = refs
    a_refs, b_refs, rest = rest[:n_a], rest[n_a : n_a + n_b], rest[n_a + n_b :]
    if last:
        out_ref, tokens, coded, logits = rest
    else:
        out_ref, tables, gains, tokens, coded, logits, scales, arrived = rest
    rows = tables.shape[0] // 2
    blocks = 2 * rows // block

    if not last:
        for k in range(blocks):
            source = (own_ref, swapped_ref)[k * block // rows]
            at = pl.ds(k * block % rows, block)
            pltpu.make_async_copy(
                source.at[at], tables.at[pl.ds(k * block, block)], arrived.at[k]
            ).start()
        scales[: rows // 128, :] = own_scale[...]
        scales[rows // 128 :, :] = swapped_scale[...]
    index = lax.axis_index("vocab")
    x, z, core = place(index)

    def spot(half, dz):
        return pl.ds(pl.multiple_of(half * HALF + lax.rem(z + dz + NZ, NZ) * ROWS, ROWS), ROWS)

    for buffer, row, column, half, dz in a_spots:
        tokens[spot(half, dz), :CA] = a_refs[buffer][row : row + ROWS, column : column + CA]
    for buffer, row, column, half, dz in b_spots:
        ref = b_refs[buffer]
        tokens[spot(half, dz), CA:] = ref[row : row + ROWS, column : column + CB]
        coded[spot(half, dz), :] = ref[row : row + ROWS, column + CB : column + CB + CT].astype(f32)
    code = coded[...].T
    target = (code[0:1, :] * 256.0 + code[1:2, :]).astype(jnp.int32)
    own_base, swapped_base = index * rows, (index - 2 * core) * rows

    def step(k, carry):
        peak, picked = carry
        part = pl.ds(pl.multiple_of(k * block, block), block)
        if not last:
            pltpu.make_async_copy(own_ref.at[pl.ds(0, block)], tables.at[part], arrived.at[k]).wait()
            for j in range(block // 128):
                some = pl.ds(pl.multiple_of(k * block + j * 128, 128), 128)
                total = jnp.zeros((128, 128), f32)
                for i in range(D // 128):
                    piece = tables[some, i * 128 : (i + 1) * 128].astype(f32)
                    total += piece * piece
                norm = lax.rsqrt(jnp.sum(total, axis=1, keepdims=True) + epsilon)
                scale = scales[pl.ds(k * (block // 128) + j, 1), :]
                gains[some, :] = norm * jnp.broadcast_to(scale, (128, 128)).T
        value = lax.dot_general(
            tables[part, :], tokens[...], (((1,), (1,)), ((), ())), preferred_element_type=f32
        )
        factor = gains[part, :]
        value = value * jnp.concatenate([factor, factor], axis=1)
        logits[part, :] = value
        base = jnp.where(k * block < rows, own_base, swapped_base) + k * block
        row = lax.broadcasted_iota(jnp.int32, (block, 256), 0)
        chosen = jnp.where(row == target - base, value, 0.0)
        peak = jnp.maximum(peak, jnp.max(value.reshape(block // 8, 8, 256), axis=0))
        picked = picked + jnp.sum(chosen.reshape(block // 8, 8, 256), axis=0)
        return peak, picked

    peak, picked = lax.fori_loop(
        0, blocks, step, (jnp.full((8, 256), -jnp.inf, f32), jnp.zeros((8, 256), f32))
    )
    peak = jnp.max(peak, axis=0, keepdims=True)

    def add(k, total):
        part = pl.ds(pl.multiple_of(k * 256, 256), 256)
        term = jnp.exp(logits[part, :] - peak)
        return total + jnp.sum(term.reshape(32, 8, 256), axis=0)

    total = lax.fori_loop(0, 2 * rows // 256, add, jnp.zeros((8, 256), f32))
    log_sum = peak + jnp.log(jnp.sum(total, axis=0, keepdims=True))
    picked = jnp.sum(picked, axis=0, keepdims=True)
    row = lax.broadcasted_iota(jnp.int32, (8, 128), 0)
    both = first_ref[...] if last else jnp.zeros((8, 128), f32)
    for half, dx in enumerate((0, 2) if last else (-1, 1)):
        xs = lax.rem(x + dx + NX, NX)
        lanes = slice(half * 128, half * 128 + 128)
        both = jnp.where(row == xs, log_sum[:, lanes], both)
        both = jnp.where(row == xs + NX, picked[:, lanes], both)
    out_ref[...] = jnp.broadcast_to(both[None], out_ref.shape) if last else both


def close_kernel(pieces_ref, loss_ref, sum_ref):
    log_sum = pieces_ref[:, :NX, :]
    peak = jnp.max(log_sum, axis=0)
    total = jnp.sum(jnp.exp(log_sum - peak[None]), axis=0)
    loss = peak + jnp.log(total) - jnp.sum(pieces_ref[:, NX:, :], axis=0)
    loss_ref[...] = loss
    summed = jnp.sum(jnp.sum(loss, axis=0, keepdims=True), axis=1, keepdims=True)
    sum_ref[...] = jnp.broadcast_to(summed[None], sum_ref.shape)


def head_loss(hidden, embedding, logit_scale, targets):
    rows = embedding.shape[0]
    index = lax.axis_index("vocab")
    x, z, _ = place(index)
    swapped = shift(embedding, 0, 0, 1)
    any_space = pl.BlockSpec(memory_space=pltpu.HBM)
    unit, a, b, own_scale = call(
        unit_kernel,
        (
            pltpu.VMEM((ROWS, D + CT), bf16),
            pltpu.VMEM((ROWS, CA), bf16),
            pltpu.VMEM((ROWS, CB + CT), bf16),
            pltpu.VMEM((rows // 128, 128), f32),
        ),
        58 << 20,
        (
            pltpu.VMEM((ROWS, D), bf16),
            pltpu.VMEM((1, ROWS), jnp.int32),
            pltpu.SemaphoreType.DMA((3,)),
        ),
        specs=[any_space] * 3,
    )(hidden, targets.reshape(1, ROWS), logit_scale.reshape(rows // 128, 128))
    swapped_scale = shift(own_scale, 0, 0, 1)

    a_far = shift(a, 2, 0)
    left, right = shift(unit, 1, 0), shift(unit, -1, 0)
    b1, c1, b2, c2 = shift(b, 0, 1), shift(b, 0, -1), shift(b, 0, 2), shift(b, 0, -2)
    line = jnp.concatenate([left[:, :CA], right[:, :CA], a, a_far])
    p1, m1 = shift(line, 0, 1), shift(line, 0, -1)
    near = jnp.concatenate([b1, c1, b2, c2])
    q1, n1 = shift(near, 1, 0), shift(near, -1, 0)
    p2, m2 = shift(line, 0, 2), shift(line, 0, -2)
    b3, c3, b4 = shift(b2, 0, 1), shift(c2, 0, -1), shift(b2, 0, 2)
    p3, m3, p4 = shift(p2, 0, 1), shift(m2, 0, -1), shift(p2, 0, 2)
    apart = jnp.concatenate([b3, c3, b4])
    q2, n2 = shift(apart, 1, 0), shift(apart, -1, 0)
    q3 = shift(q1, 1, 0)
    n3 = shift(jnp.concatenate([right[:, CA:], n2]), -1, 0)

    lines = (line, p1, m1, p2, m2, p3, m3, p4)
    line_dz = (0, -1, 1, -2, 2, -3, 3, -4)
    near_dz, apart_dz = (-1, 1, -2, 2), (-3, 3, -4)

    def spots(buffer, half, offsets, column=0):
        return [(buffer, k * ROWS, column, half, dz) for k, dz in enumerate(offsets)]

    cost = pl.CostEstimate(
        flops=2 * 2 * rows * D * 256, bytes_accessed=16 * rows * D, transcendentals=0
    )
    scratch = (
        pltpu.VMEM((256, D), bf16),
        pltpu.VMEM((256, CT), f32),
        pltpu.VMEM((2 * rows, 256), f32),
    )

    def head(a_spots, b_spots, given, specs, sources, name):
        last = name == "head_column"
        piece = jax.ShapeDtypeStruct((NX * NZ, 8, 128) if last else (8, 128), f32)
        kept = (pltpu.VMEM((2 * rows, D), bf16), pltpu.VMEM((2 * rows, 128), f32))
        more = (
            pltpu.VMEM((2 * rows // 128, 128), f32),
            pltpu.SemaphoreType.DMA((2 * rows // BLOCK,)),
        )
        return call(
            functools.partial(head_kernel, a_spots, b_spots, last, (len(lines), len(sources))),
            piece if last else (piece, *kept),
            28 << 20,
            scratch if last else scratch + more,
            cost,
            specs + [VMEM] * (len(lines) + len(sources)),
        )(*given, *lines, *sources)

    a_spots = [(k, half * ROWS, 0, half, dz) for k, dz in enumerate(line_dz) for half in (0, 1)]
    b_spots = []
    for half in (0, 1):
        b_spots += spots(3 * half, half, (0,), CA)
        b_spots += spots(3 * half + 1, half, near_dz)
        b_spots += spots(3 * half + 2, half, apart_dz)
    sides = (left, q1, q2, right, n1, n2)
    given = (embedding, swapped, own_scale, swapped_scale)
    specs = [any_space] * 2 + [VMEM] * 2
    first, tables, gains = head(a_spots, b_spots, given, specs, sides, "head_sides")
    a_spots = [
        (k, (2 + half) * ROWS, 0, half, dz) for k, dz in enumerate(line_dz) for half in (0, 1)
    ]
    b_spots = spots(0, 0, (0,)) + spots(1, 0, near_dz) + spots(2, 0, apart_dz)
    b_spots += spots(3, 1, near_dz) + spots(4, 1, (0,) + apart_dz)
    columns = (b, near, apart, q3, n3)
    given = (tables, gains, first)
    pieces = head(a_spots, b_spots, given, [VMEM] * 3, columns, "head_column")

    same_core = [[v for v in range(NX * NZ * NC) if v % NC == c] for c in range(NC)]
    pieces = lax.all_to_all(pieces, "vocab", 0, 0, tiled=True, axis_index_groups=same_core)
    loss, summed = call(
        close_kernel,
        (jax.ShapeDtypeStruct((NX, 128), f32), jax.ShapeDtypeStruct((NY * NC, 1, 128), f32)),
        4 << 20,
    )(pieces)
    groups = [
        [(v + c) * NY + s for c in range(NC) for s in range(NY)]
        for v in range(0, NX * NZ * NC, NC)
    ]
    summed = lax.all_to_all(summed, ("vocab", "seq"), 0, 0, tiled=True, axis_index_groups=groups)
    mean_loss = jnp.sum(summed[:, 0, 0]) / (NX * NZ * NC * NY * ROWS)
    own_loss = lax.dynamic_slice(loss, (x, z * ROWS), (1, ROWS)).reshape(ROWS)
    return own_loss, mean_loss


def solution(mesh):
    in_specs = (P(("vocab", "seq"), None), P("vocab", None), P("vocab"), P(("vocab", "seq")))
    out_specs = (P(("vocab", "seq")), P())
    return jax.shard_map(
        head_loss, mesh=mesh, in_specs=in_specs, out_specs=out_specs, check_vma=False
    )
```
